32 devices in a mesh: groups: 2 (over x), ref: 16 (over z, y, core).
Axes of the slice: x: 2, y: 2, z: 4, core: 2. Of those that a mesh axis runs over, the one named last changes fastest.
Arguments:
- long_series: bfloat16 [131072], P(('groups', 'ref')), parts along dimension 0, may hold values from -12 to 12
- queries: bfloat16 [64, 1024], P(('groups', 'ref')), parts along dimension 0, may hold values from -48 to 48
- lengths: int32 [64], P(('groups', 'ref')), parts along dimension 0, may hold values from 512 to 1024, as said below
- groups: int32 [64], P(('groups', 'ref')), parts along dimension 0, may hold values from 0 to 15, as said below
Outputs:
- profile: float32 [64, 1024], P(('groups', 'ref')), parts along dimension 0
The draws below stay inside these ranges and needn't reach their ends.
There are 2 independent parts, one for each index of `groups`. The reference program is written for one: setup_inputs(seed, part) draws one part's arguments, and reference() takes and returns one part's arrays. A program takes and returns all parts, laid end to end along the dimension named above; each array names one. Nothing has to cross between parts.
Inputs may be any that keep to these rules, and one draw needn't show every extreme that they name: `lengths`: multiples of 128. `groups`: region g holds reference blocks g * 1 to (g + 1) * 1 - 1; at most 4 queries name one region, and one region is named by exactly 4.
All inputs are finite; a program needn't handle non-finite values.
Results may differ from the reference program's by a relative error of at most 0.0003.
Values may be sent and summed in bfloat16 or wider, within the bound.
A program may use at most 64 MiB of HBM per device.

```python
import math
import jax
import jax.numpy as jnp
from jax import lax

M = 256
LQ = 1024
RDEV = 4096
GDEV = 1
RMAX = 4
NQ = 32
NR = 65536
NGRP = 16


def make_join(key):
    blocks = NR // 128
    values = jax.random.normal(jax.random.fold_in(key, 1), (NR,), jnp.float32)
    shifts = 0.5 * jax.random.normal(jax.random.fold_in(key, 2), (blocks,), jnp.float32)
    scales = jnp.exp(jax.random.uniform(jax.random.fold_in(key, 3), (blocks,), jnp.float32, math.log(0.5), math.log(2.0)))
    series = jnp.clip(values * jnp.repeat(scales, 128) + jnp.repeat(shifts, 128), -12.0, 12.0)
    order = jax.random.permutation(jax.random.fold_in(key, 4), NQ)
    position = jnp.argsort(order)
    leader = jax.random.randint(jax.random.fold_in(key, 5), (), 0, NGRP)
    others = (leader + 1 + (position - RMAX) % (NGRP - 1)) % NGRP
    groups = jnp.where(position < RMAX, leader, others).astype(jnp.int32)
    copies = LQ // M
    starts = groups[:, None] * (GDEV * RDEV) + jax.random.randint(jax.random.fold_in(key, 6), (NQ, copies), 0, GDEV * RDEV - M + 1)
    gather_index = (starts[:, :, None] + jnp.arange(M, dtype=jnp.int32)[None, None, :]).reshape(NQ, LQ)
    copied = series[gather_index]
    noise_level = jnp.exp(jax.random.uniform(jax.random.fold_in(key, 7), (NQ, LQ // 128), jnp.float32, math.log(0.05), math.log(3.0)))
    noise = jax.random.normal(jax.random.fold_in(key, 8), (NQ, LQ), jnp.float32)
    made = copied + jnp.repeat(noise_level, 128, axis=1) * noise
    return (series, jnp.clip(made, -48.0, 48.0), groups)


def draw_long_series(key, part):
    return make_join(key)[0].astype(jnp.bfloat16)


def draw_queries(key, part):
    return make_join(key)[1].astype(jnp.bfloat16)


def draw_groups(key, part):
    return make_join(key)[2]


def draw_lengths(key, part):
    units = jax.random.randint(jax.random.fold_in(key, 31), (NQ,), LQ // 256, LQ // 128 + 1)
    sized = 128 * units
    return sized.at[0].set(LQ).at[1].set(LQ // 2).astype(jnp.int32)


def setup_inputs(seed: int = 0, part: int = 0) -> dict:
    keys = jax.random.split(jax.random.key(seed), 5)
    own_keys = jax.random.split(jax.random.fold_in(keys[4], part), 5)
    long_series = draw_long_series(jax.random.fold_in(jax.random.fold_in(keys[4], part), 71), part)
    queries = draw_queries(jax.random.fold_in(jax.random.fold_in(keys[4], part), 71), part)
    lengths = draw_lengths(jax.random.fold_in(jax.random.fold_in(keys[4], part), 71), part)
    groups = draw_groups(jax.random.fold_in(jax.random.fold_in(keys[4], part), 71), part)
    return dict(long_series=long_series, queries=queries, lengths=lengths, groups=groups)


SPREAD_FLOOR = 0.25

def window_stats(series, count):
    offsets_grid = jnp.arange(count, dtype=jnp.int32)[:, None] + jnp.arange(M, dtype=jnp.int32)[None, :]
    windows = series[offsets_grid]
    values = windows.astype(jnp.float32)
    centre = lax.optimization_barrier(jnp.mean(values, axis=1))
    spread = jnp.sqrt(lax.optimization_barrier(jnp.mean((values - centre[:, None]) ** 2, axis=1)) + SPREAD_FLOOR)
    return (windows, centre, spread)

def best_match(query_set, ref_set, usable):
    query_windows, query_centre, query_spread = query_set
    ref_windows, ref_centre, ref_spread = ref_set
    products = lax.dot_general(query_windows.astype(jnp.float32), ref_windows.astype(jnp.float32), (((1,), (1,)), ((), ())), precision=lax.Precision.HIGHEST, preferred_element_type=jnp.float32)
    correlation = (products - M * query_centre[:, None] * ref_centre[None, :]) / (M * query_spread[:, None] * ref_spread[None, :])
    correlation = jnp.where(usable[None, :], correlation, -2.0)
    return lax.optimization_barrier(jnp.max(correlation, axis=1))

def reference(long_series, queries, lengths, groups):
    overall = long_series.shape[0]
    padded = jnp.concatenate([long_series, jnp.zeros((M,), jnp.bfloat16)])

    def match_query(entry_pair):
        series, region = entry_pair
        query_set = window_stats(jnp.concatenate([series, jnp.zeros((M,), jnp.bfloat16)]), LQ)
        best_so_far = jnp.full((LQ,), -2.0, jnp.float32)
        for offset in range(GDEV):
            block_index = region * GDEV + offset
            first_cell = (block_index * RDEV).astype(jnp.int32)
            segment = lax.dynamic_slice_in_dim(padded, first_cell, RDEV + M)
            ref_set = window_stats(segment, RDEV)
            usable = first_cell + jnp.arange(RDEV, dtype=jnp.int32) <= overall - M
            best_so_far = jnp.maximum(best_so_far, best_match(query_set, ref_set, usable))
        return best_so_far
    best_values = lax.map(match_query, (queries, groups))
    live_points = jnp.arange(LQ, dtype=jnp.int32)[None, :] <= lengths[:, None] - M
    return jnp.where(live_points, 2.0 * (1.0 - best_values), 0.0)
```

```python
import functools

import jax
import jax.numpy as jnp
from jax import lax
from jax.experimental import pallas as pl
from jax.experimental.pallas import tpu as pltpu
from jax.sharding import PartitionSpec as P

M = 256
LANES = 128
WIDE = 2 * LANES
SPREAD_FLOOR = 0.25
CHUNK = 4
PIECE = 16
MASKED = -1e30


def iotas(shape):
    return (
        lax.broadcasted_iota(jnp.int32, shape, 0),
        lax.broadcasted_iota(jnp.int32, shape, 1),
    )


def hankel_tiles(rows):
    shape = (LANES, LANES)
    sub, lane = iotas(shape)
    rolled = [
        pltpu.roll(jnp.broadcast_to(row, shape), 1, 1, stride=1, stride_axis=0) for row in rows
    ]
    return [
        jnp.where(lane <= sub, here, there).astype(jnp.bfloat16)
        for here, there in zip(rolled, rolled[1:])
    ]


def toeplitz(row, following):
    shape = (LANES, LANES)
    sub, lane = iotas(shape)
    here = pltpu.roll(jnp.broadcast_to(row, shape), 0, 1, stride=1, stride_axis=0)
    there = pltpu.roll(jnp.broadcast_to(following, shape), 0, 1, stride=1, stride_axis=0)
    return jnp.where(lane >= sub, here, there)


def next_row(x):
    return pltpu.roll(x, x.shape[0] - 1, 0)


def window_scale(x):
    lane = lax.broadcasted_iota(jnp.int32, x.shape, 1)
    total, square = x, jnp.zeros_like(x)
    count = 1
    while count < M:
        def ahead(v):
            if count == LANES:
                return next_row(v)
            rolled = pltpu.roll(v, LANES - count, 1)
            return jnp.where(lane < LANES - count, rolled, next_row(rolled))

        total_ahead, square_ahead = ahead(total), ahead(square)
        gap = total - total_ahead
        square = square + square_ahead + gap * gap * (0.5 / count)
        total = total + total_ahead
        count *= 2
    return 1.0 / jnp.sqrt(square * (1.0 / M) + SPREAD_FLOOR)


def join_kernel(members, groups_hbm, lengths_hbm, q_hbm, block_hbm, out_ref,
                series_ref, left_ref, mean_ref, points_ref, total_ref, scale_ref,
                q_scale_ref, acc_ref, q_ref, groups_ref, lengths_ref,
                local_sem, send_sem, recv_sem):
    tall = left_ref.shape[1]
    pieces = tall // PIECE
    specs = [pltpu.ACC(x)((PIECE, WIDE), jnp.float32) for x in range(2) for _ in range(pieces)]

    def main(*accs):
        join_body(members, groups_hbm, lengths_hbm, q_hbm, block_hbm, out_ref,
                  series_ref, left_ref, mean_ref, points_ref, total_ref, scale_ref,
                  q_scale_ref, acc_ref, q_ref, groups_ref, lengths_ref,
                  local_sem, send_sem, recv_sem, (accs[:pieces], accs[pieces:]))

    pl.run_scoped(main, *specs)


def join_body(members, groups_hbm, lengths_hbm, q_hbm, block_hbm, out_ref,
              series_ref, left_ref, mean_ref, points_ref, total_ref, scale_ref,
              q_scale_ref, acc_ref, q_ref, groups_ref, lengths_ref,
              local_sem, send_sem, recv_sem, accs):
    per_device, series_len = q_ref.shape
    q_rows = series_len // LANES
    rows = block_hbm.shape[0]
    full = (series_len - M) // LANES
    tall = left_ref.shape[1]
    pieces = tall // PIECE
    q_pad = q_rows + 8
    chunks = rows // CHUNK
    me = lax.axis_index("ref")

    def place(d):
        return lax.rem(me + d, members)

    def slot(owner):
        return series_ref.at[owner]

    def copy(src, d):
        return pltpu.make_async_remote_copy(
            src_ref=src, dst_ref=src, send_sem=send_sem.at[0], recv_sem=recv_sem.at[0],
            device_id={"ref": place(d)}, device_id_type=pl.DeviceIdType.MESH,
        )

    fetches = [
        pltpu.make_async_copy(block_hbm, slot(me), local_sem.at[0]),
        pltpu.make_async_copy(q_hbm, q_ref, local_sem.at[1]),
        pltpu.make_async_copy(groups_hbm, groups_ref, local_sem.at[2]),
        pltpu.make_async_copy(lengths_hbm, lengths_ref, local_sem.at[3]),
    ]
    barrier = pltpu.get_barrier_semaphore()
    for fetch in fetches:
        fetch.start()

    @pl.loop(1, members)
    def _(d):
        pl.semaphore_signal(
            barrier, inc=1, device_id={"ref": place(d)}, device_id_type=pl.DeviceIdType.MESH
        )

    series_ref[members] = jnp.zeros((rows, LANES), jnp.bfloat16)
    acc_ref[...] = jnp.full(acc_ref.shape, MASKED, jnp.float32)
    fetches[0].wait()
    pl.semaphore_wait(barrier, members - 1)

    @pl.loop(1, members)
    def _(d):
        copy(slot(me), d).start()

    fetches[1].wait()
    fetches[2].wait()
    fetches[3].wait()

    sub, lane = iotas((WIDE, WIDE))
    flip = jnp.where(sub + lane == LANES - 1, 1.0, 0.0).astype(jnp.bfloat16)
    ones = jnp.full((WIDE, WIDE), 1.0 / M, jnp.bfloat16)
    q_all = q_ref[...].astype(jnp.float32)
    parts = []
    for p in range(per_device):
        row_list = [q_all[p : p + 1, LANES * a : LANES * (a + 1)] for a in range(q_rows)]
        parts += row_list + [jnp.zeros((q_pad - q_rows, LANES), jnp.float32)]
    q_points = jnp.concatenate(parts, axis=0)
    q_scale_ref[...] = window_scale(q_points)
    q_lhs = jnp.concatenate([q_points, jnp.zeros_like(q_points)], axis=1).astype(jnp.bfloat16)
    pltpu.matmul_push_rhs(flip, 0, 0)
    for p in range(per_device):
        pltpu.matmul_acc_lhs(
            accs[0][p], q_lhs[p * q_pad : (p + 1) * q_pad], load_staged_rhs=None if p else 0
        )
    for x in range(2):
        pltpu.matmul_push_rhs(ones, 0, x)
    for p in range(per_device):
        q_back = pltpu.matmul_pop(accs[0][p])[:, :LANES]
        for a in range(full + 2):
            tile = toeplitz(q_back[a : a + 1], q_back[a + 1 : a + 2]).astype(jnp.bfloat16)
            for h in range(2):
                if 0 <= a - h < full:
                    left_ref[p, pl.ds((a - h) * LANES, LANES), pl.ds(h * LANES, LANES)] = tile
                elif a - h == full:
                    left_ref[p, pl.ds(full * LANES, PIECE), pl.ds(h * LANES, LANES)] = tile[:PIECE]
    for p in range(per_device):
        for i in range(pieces):
            x = i % 2
            pltpu.matmul_acc_lhs(
                accs[x][i], left_ref[p, pl.ds(i * PIECE, PIECE), :],
                load_staged_rhs=0 if p == 0 and i < 2 else None,
            )
        for i in range(pieces):
            mean_ref[p, pl.ds(i * PIECE, PIECE), :] = pltpu.matmul_pop(accs[i % 2][i])[:, :LANES]

    near = jnp.where((lane >= LANES) | (sub >= LANES) | (sub >= lane), 1.0, 0.0).astype(jnp.bfloat16)
    far = jnp.where((sub < LANES) & (sub < lane), 1.0, 0.0).astype(jnp.bfloat16)
    for x in range(2):
        pltpu.matmul_push_rhs(near, 0, x)
        pltpu.matmul_push_rhs(far, 1, x)

    whole = series_ref.at[pl.ds(0, members - 1)]
    copy(whole, 1).wait_recv()

    for p in range(per_device):
        g = groups_ref[p]
        block = series_ref[g].astype(jnp.float32)
        ahead = series_ref[g + 1].astype(jnp.float32)
        points_ref[p, pl.ds(0, rows), :] = block
        points_ref[p, pl.ds(rows, 8), :] = ahead[:8]
        shape = (8, LANES)
        spot = lax.broadcasted_iota(jnp.int32, shape, 1)
        tail = jnp.concatenate([block[rows - 2 :], ahead[:6]], axis=0)
        moved = pltpu.roll(block[rows - 8 :], LANES - 1, 1)
        moved = jnp.where(spot < LANES - 1, moved, next_row(moved))
        moved = jnp.concatenate([moved[4:], moved[:4]], axis=0)
        final = jnp.full(shape, g, jnp.int32) == members - 1
        points_ref[p, pl.ds(rows + 8, 8), :] = jnp.where(final, moved, tail)
    for p in range(per_device):
        x = p % 2
        here, ahead, beyond = (points_ref[p, pl.ds(s, rows + PIECE), :] for s in range(3))

        def operand(f):
            close = jnp.concatenate([f(here), f(ahead)], axis=1)
            away = jnp.concatenate([f(beyond), jnp.zeros_like(f(beyond))], axis=1)
            return close, away

        def high(v):
            return (v * v).astype(jnp.bfloat16)

        def low(v):
            return (v * v - high(v).astype(jnp.float32)).astype(jnp.bfloat16)

        plain = operand(lambda v: v.astype(jnp.bfloat16))
        squares = [operand(high), operand(low)]
        stat_pieces = rows // PIECE + 1
        for s in range(2):
            for t in range(stat_pieces):
                cut = slice(t * PIECE, (t + 1) * PIECE)
                pltpu.matmul_acc_lhs(
                    accs[x][2 * t], plain[s][cut], load_staged_rhs=s if t == 0 else None
                )
                for square in squares:
                    pltpu.matmul_acc_lhs(accs[x][2 * t + 1], square[s][cut])
        for t in range(stat_pieces):
            total = pltpu.matmul_pop(accs[x][2 * t])[:, :LANES]
            square = pltpu.matmul_pop(accs[x][2 * t + 1])[:, :LANES]
            mean = total * (1.0 / M)
            spread = jnp.maximum(square * (1.0 / M) - mean * mean, 0.0)
            total_ref[p, pl.ds(t * PIECE, PIECE), :] = total
            scale_ref[p, pl.ds(t * PIECE, PIECE), :] = 1.0 / jnp.sqrt(spread + SPREAD_FLOOR)

    half = rows // 2

    def starts(c):
        return 2 * c, jnp.where(c == chunks - 1, rows + 8, half + 2 * c)

    def push(k):
        p, c = k // chunks, k % chunks
        for x, first in enumerate(starts(c)):
            tiles = hankel_tiles([points_ref[p, pl.ds(first + m, 1), :] for m in range(4)])
            rhs = jnp.concatenate(
                [
                    jnp.concatenate([tiles[0], tiles[1]], axis=1),
                    jnp.concatenate([tiles[1], tiles[2]], axis=1),
                ],
                axis=0,
            )
            pltpu.matmul_push_rhs(rhs, 0, x)

    third = -(-pieces // 3)
    parts = [range(s, min(s + third, pieces)) for s in range(0, pieces, third)]

    def multiply(k, part):
        for i in parts[part]:
            lhs = left_ref[k // chunks, pl.ds(i * PIECE, PIECE), :]
            for x in range(2):
                pltpu.matmul_acc_lhs(accs[x][i], lhs, load_staged_rhs=None if i else 0)

    def fold(k, part):
        p, c = k // chunks, k % chunks
        at_rows = [first + n for first in starts(c) for n in range(2)]
        totals = [total_ref[p, pl.ds(at, 1), :] for at in at_rows]
        scales = [scale_ref[p, pl.ds(at, 1), :] for at in at_rows]
        for i in parts[part]:
            at = pl.ds(i * PIECE, PIECE)
            mean = mean_ref[p, at, :]
            popped = [pltpu.matmul_pop(accs[x][i]) for x in range(2)]
            best = acc_ref[p, at, :]
            for n in range(CHUNK):
                piece = popped[n // 2][:, (n % 2) * LANES : (n % 2 + 1) * LANES]
                best = jnp.maximum(best, (piece - mean * totals[n]) * scales[n])
            acc_ref[p, at, :] = best

    def finish(p):
        spot = lax.broadcasted_iota(jnp.int32, (1, LANES), 1)
        limit = lengths_ref[p] - M
        for a in range(q_rows):
            if a < full:
                block = acc_ref[p, pl.ds(a * LANES, LANES), :]
                best = jnp.max(block.T, axis=0, keepdims=True)
            elif a == full:
                block = acc_ref[p, pl.ds(a * LANES, 8), :]
                best = jnp.broadcast_to(jnp.max(block, axis=1, keepdims=True)[:1], (1, LANES))
            if a <= full:
                best = best * q_scale_ref[pl.ds(p * q_pad + a, 1), :] * (1.0 / M)
                row = jnp.where(a * LANES + spot <= limit, 2.0 * (1.0 - best), 0.0)
            else:
                row = jnp.zeros((1, LANES), jnp.float32)
            out_ref[pl.ds(p, 1), pl.ds(a * LANES, LANES)] = row

    steps = per_device * chunks
    push(0)
    multiply(0, 0)
    multiply(0, 1)
    multiply(0, 2)
    push(1)
    fold(0, 0)

    @pl.loop(1, steps)
    def _(k):
        multiply(k, 0)
        fold(k - 1, 1)
        multiply(k, 1)
        fold(k - 1, 2)
        multiply(k, 2)
        push(lax.rem(k + 1, steps))
        fold(k, 0)

    fold(steps - 1, 1)
    fold(steps - 1, 2)
    for x in range(2):
        pltpu.matmul_acc_lhs(accs[x][0], left_ref[0, pl.ds(0, PIECE), :], load_staged_rhs=0)
        pltpu.matmul_pop(accs[x][0])
    for p in range(per_device):
        finish(p)
    copy(whole, 1).wait_send()


def join(members, groups, lengths, queries, block):
    per_device, series_len = queries.shape
    rows = block.shape[0]
    tall = (series_len - M) // LANES * LANES + PIECE
    q_rows = per_device * (series_len // LANES + 8)
    vmem = pl.BlockSpec(memory_space=pltpu.VMEM)
    return pl.pallas_call(
        functools.partial(join_kernel, members),
        out_shape=pltpu.VMEM((per_device, series_len), jnp.float32),
        in_specs=[pl.BlockSpec(memory_space=pl.ANY)] * 4,
        out_specs=vmem,
        scratch_shapes=[
            pltpu.VMEM((members + 1, rows, LANES), jnp.bfloat16),
            pltpu.VMEM((per_device, tall, M), jnp.bfloat16),
            pltpu.VMEM((per_device, tall, LANES), jnp.float32),
            pltpu.VMEM((per_device, rows + 24, LANES), jnp.float32),
            pltpu.VMEM((per_device, rows + PIECE, LANES), jnp.float32),
            pltpu.VMEM((per_device, rows + PIECE, LANES), jnp.float32),
            pltpu.VMEM((q_rows, LANES), jnp.float32),
            pltpu.VMEM((per_device, tall, LANES), jnp.float32),
            pltpu.VMEM((per_device, series_len), jnp.bfloat16),
            pltpu.SMEM((per_device,), jnp.int32),
            pltpu.SMEM((per_device,), jnp.int32),
            pltpu.SemaphoreType.DMA((4,)),
            pltpu.SemaphoreType.DMA((1,)),
            pltpu.SemaphoreType.DMA((1,)),
        ],
        compiler_params=pltpu.CompilerParams(collective_id=0, has_side_effects=True),
        name="join",
    )(groups, lengths, queries, block)


def body(long_series, queries, lengths, groups):
    members = lax.axis_size("ref")
    return join(members, groups, lengths, queries, long_series.reshape(-1, LANES))


def solution(mesh):
    in_specs = (
        P(("groups", "ref")),
        P(("groups", "ref"), None),
        P(("groups", "ref")),
        P(("groups", "ref")),
    )
    out_specs = P(("groups", "ref"), None)
    return jax.shard_map(body, mesh=mesh, in_specs=in_specs, out_specs=out_specs, check_vma=False)
```

```python
import functools

import jax
import jax.numpy as jnp
from jax import lax
from jax.experimental import pallas as pl
from jax.experimental.pallas import tpu as pltpu
from jax.sharding import PartitionSpec as P

M = 256
LANES = 128
WIDE = 2 * LANES
SPREAD_FLOOR = 0.25
CHUNK = 4
PIECE = 16
MASKED = -1e30


def iotas(shape):
    return (
        lax.broadcasted_iota(jnp.int32, shape, 0),
        lax.broadcasted_iota(jnp.int32, shape, 1),
    )


def hankel_tiles(rows):
    shape = (LANES, LANES)
    sub, lane = iotas(shape)
    rolled = [
        pltpu.roll(
            jnp.broadcast_to(row, shape).astype(jnp.bfloat16), 1, 1, stride=1, stride_axis=0
        )
        for row in rows
    ]
    return [
        jnp.where(lane <= sub, here, there) for here, there in zip(rolled, rolled[1:])
    ]


def toeplitz(row, following):
    shape = (LANES, LANES)
    sub, lane = iotas(shape)
    here = pltpu.roll(jnp.broadcast_to(row, shape), 0, 1, stride=1, stride_axis=0)
    there = pltpu.roll(jnp.broadcast_to(following, shape), 0, 1, stride=1, stride_axis=0)
    return jnp.where(lane >= sub, here, there)


def next_row(x):
    return pltpu.roll(x, x.shape[0] - 1, 0)


def window_scale(x):
    lane = lax.broadcasted_iota(jnp.int32, x.shape, 1)
    total, square = x, jnp.zeros_like(x)
    count = 1
    while count < M:
        def ahead(v):
            if count == LANES:
                return next_row(v)
            rolled = pltpu.roll(v, LANES - count, 1)
            return jnp.where(lane < LANES - count, rolled, next_row(rolled))

        total_ahead, square_ahead = ahead(total), ahead(square)
        gap = total - total_ahead
        square = square + square_ahead + gap * gap * (0.5 / count)
        total = total + total_ahead
        count *= 2
    return 1.0 / jnp.sqrt(square * (1.0 / M) + SPREAD_FLOOR)


def join_kernel(members, groups_hbm, lengths_hbm, q_hbm, block_hbm, out_ref,
                series_ref, left_ref, mean_ref, points_ref, total_ref, scale_ref,
                q_scale_ref, acc_ref, q_ref, groups_ref, lengths_ref,
                local_sem, send_sem, recv_sem):
    tall = left_ref.shape[1]
    pieces = tall // PIECE
    specs = [pltpu.ACC(x)((PIECE, WIDE), jnp.float32) for x in range(2) for _ in range(pieces)]

    def main(*accs):
        join_body(members, groups_hbm, lengths_hbm, q_hbm, block_hbm, out_ref,
                  series_ref, left_ref, mean_ref, points_ref, total_ref, scale_ref,
                  q_scale_ref, acc_ref, q_ref, groups_ref, lengths_ref,
                  local_sem, send_sem, recv_sem, (accs[:pieces], accs[pieces:]))

    pl.run_scoped(main, *specs)


def join_body(members, groups_hbm, lengths_hbm, q_hbm, block_hbm, out_ref,
              series_ref, left_ref, mean_ref, points_ref, total_ref, scale_ref,
              q_scale_ref, acc_ref, q_ref, groups_ref, lengths_ref,
              local_sem, send_sem, recv_sem, accs):
    per_device, series_len = q_ref.shape
    q_rows = series_len // LANES
    rows = block_hbm.shape[0]
    full = (series_len - M) // LANES
    tall = left_ref.shape[1]
    pieces = tall // PIECE
    q_pad = q_rows + 8
    chunks = rows // CHUNK
    me = lax.axis_index("ref")

    def place(d):
        return lax.rem(me + d, members)

    def slot(owner):
        return series_ref.at[owner]

    def copy(src, d):
        return pltpu.make_async_remote_copy(
            src_ref=src, dst_ref=src, send_sem=send_sem.at[0], recv_sem=recv_sem.at[0],
            device_id={"ref": place(d)}, device_id_type=pl.DeviceIdType.MESH,
        )

    fetches = [
        pltpu.make_async_copy(block_hbm, slot(me), local_sem.at[0]),
        pltpu.make_async_copy(q_hbm, q_ref, local_sem.at[1]),
        pltpu.make_async_copy(groups_hbm, groups_ref, local_sem.at[2]),
        pltpu.make_async_copy(lengths_hbm, lengths_ref, local_sem.at[3]),
    ]
    barrier = pltpu.get_barrier_semaphore()
    for fetch in fetches:
        fetch.start()

    @pl.loop(1, members)
    def _(d):
        pl.semaphore_signal(
            barrier, inc=1, device_id={"ref": place(d)}, device_id_type=pl.DeviceIdType.MESH
        )

    series_ref[members] = jnp.zeros((rows, LANES), jnp.bfloat16)
    acc_ref[...] = jnp.full(acc_ref.shape, MASKED, jnp.float32)
    fetches[0].wait()
    pl.semaphore_wait(barrier, members - 1)

    @pl.loop(1, members)
    def _(d):
        copy(slot(me), d).start()

    fetches[1].wait()
    fetches[2].wait()
    fetches[3].wait()

    sub, lane = iotas((WIDE, WIDE))
    flip = jnp.where(sub + lane == LANES - 1, 1.0, 0.0).astype(jnp.bfloat16)
    ones = jnp.full((WIDE, WIDE), 1.0 / M, jnp.bfloat16)
    q_all = q_ref[...].astype(jnp.float32)
    parts = []
    for p in range(per_device):
        row_list = [q_all[p : p + 1, LANES * a : LANES * (a + 1)] for a in range(q_rows)]
        parts += row_list + [jnp.zeros((q_pad - q_rows, LANES), jnp.float32)]
    q_points = jnp.concatenate(parts, axis=0)
    q_scale_ref[...] = window_scale(q_points)
    q_lhs = jnp.concatenate([q_points, jnp.zeros_like(q_points)], axis=1).astype(jnp.bfloat16)
    pltpu.matmul_push_rhs(flip, 0, 0)
    for p in range(per_device):
        pltpu.matmul_acc_lhs(
            accs[0][p], q_lhs[p * q_pad : (p + 1) * q_pad], load_staged_rhs=None if p else 0
        )
    for x in range(2):
        pltpu.matmul_push_rhs(ones, 0, x)
    for p in range(per_device):
        q_back = pltpu.matmul_pop(accs[0][p])[:, :LANES]
        for a in range(full + 2):
            tile = toeplitz(q_back[a : a + 1], q_back[a + 1 : a + 2]).astype(jnp.bfloat16)
            for h in range(2):
                if 0 <= a - h < full:
                    left_ref[p, pl.ds((a - h) * LANES, LANES), pl.ds(h * LANES, LANES)] = tile
                elif a - h == full:
                    left_ref[p, pl.ds(full * LANES, PIECE), pl.ds(h * LANES, LANES)] = tile[:PIECE]
    for p in range(per_device):
        for i in range(pieces):
            x = i % 2
            pltpu.matmul_acc_lhs(
                accs[x][i], left_ref[p, pl.ds(i * PIECE, PIECE), :],
                load_staged_rhs=0 if p == 0 and i < 2 else None,
            )
        for i in range(pieces):
            mean_ref[p, pl.ds(i * PIECE, PIECE), :] = pltpu.matmul_pop(accs[i % 2][i])[:, :LANES]

    near = jnp.where((lane >= LANES) | (sub >= LANES) | (sub >= lane), 1.0, 0.0).astype(jnp.bfloat16)
    far = jnp.where((sub < LANES) & (sub < lane), 1.0, 0.0).astype(jnp.bfloat16)
    for x in range(2):
        pltpu.matmul_push_rhs(near, 0, x)
        pltpu.matmul_push_rhs(far, 1, x)

    whole = series_ref.at[pl.ds(0, members - 1)]
    copy(whole, 1).wait_recv()

    for p in range(per_device):
        g = groups_ref[p]
        block = series_ref[g].astype(jnp.float32)
        ahead = series_ref[g + 1].astype(jnp.float32)
        points_ref[p, pl.ds(0, rows), :] = block
        points_ref[p, pl.ds(rows, 8), :] = ahead[:8]
        shape = (8, LANES)
        spot = lax.broadcasted_iota(jnp.int32, shape, 1)
        tail = jnp.concatenate([block[rows - 2 :], ahead[:6]], axis=0)
        moved = pltpu.roll(block[rows - 8 :], LANES - 1, 1)
        moved = jnp.where(spot < LANES - 1, moved, next_row(moved))
        moved = jnp.concatenate([moved[4:], moved[:4]], axis=0)
        final = jnp.full(shape, g, jnp.int32) == members - 1
        points_ref[p, pl.ds(rows + 8, 8), :] = jnp.where(final, moved, tail)
    for p in range(per_device):
        x = p % 2
        here, ahead, beyond = (points_ref[p, pl.ds(s, rows + PIECE), :] for s in range(3))

        def operand(f):
            close = jnp.concatenate([f(here), f(ahead)], axis=1)
            away = jnp.concatenate([f(beyond), jnp.zeros_like(f(beyond))], axis=1)
            return close, away

        def high(v):
            return (v * v).astype(jnp.bfloat16)

        def low(v):
            return (v * v - high(v).astype(jnp.float32)).astype(jnp.bfloat16)

        plain = operand(lambda v: v.astype(jnp.bfloat16))
        squares = [operand(high), operand(low)]
        stat_pieces = rows // PIECE + 1
        for s in range(2):
            for t in range(stat_pieces):
                cut = slice(t * PIECE, (t + 1) * PIECE)
                pltpu.matmul_acc_lhs(
                    accs[x][2 * t], plain[s][cut], load_staged_rhs=s if t == 0 else None
                )
                for square in squares:
                    pltpu.matmul_acc_lhs(accs[x][2 * t + 1], square[s][cut])
        for t in range(stat_pieces):
            total = pltpu.matmul_pop(accs[x][2 * t])[:, :LANES]
            square = pltpu.matmul_pop(accs[x][2 * t + 1])[:, :LANES]
            mean = total * (1.0 / M)
            spread = jnp.maximum(square * (1.0 / M) - mean * mean, 0.0)
            total_ref[p, pl.ds(t * PIECE, PIECE), :] = total
            scale_ref[p, pl.ds(t * PIECE, PIECE), :] = 1.0 / jnp.sqrt(spread + SPREAD_FLOOR)

    half = rows // 2

    def starts(c):
        return 2 * c, jnp.where(c == chunks - 1, rows + 8, half + 2 * c)

    def push(k):
        p, c = k // chunks, k % chunks
        for x, first in enumerate(starts(c)):
            tiles = hankel_tiles([points_ref[p, pl.ds(first + m, 1), :] for m in range(4)])
            rhs = jnp.concatenate(
                [
                    jnp.concatenate([tiles[0], tiles[1]], axis=1),
                    jnp.concatenate([tiles[1], tiles[2]], axis=1),
                ],
                axis=0,
            )
            pltpu.matmul_push_rhs(rhs, 0, x)

    third = -(-pieces // 3)
    parts = [range(s, min(s + third, pieces)) for s in range(0, pieces, third)]

    def multiply(k, part):
        for i in parts[part]:
            lhs = left_ref[k // chunks, pl.ds(i * PIECE, PIECE), :]
            for x in range(2):
                pltpu.matmul_acc_lhs(accs[x][i], lhs, load_staged_rhs=None if i else 0)

    def fold(k, part):
        p, c = k // chunks, k % chunks
        at_rows = [first + n for first in starts(c) for n in range(2)]
        totals = [total_ref[p, pl.ds(at, 1), :] for at in at_rows]
        scales = [scale_ref[p, pl.ds(at, 1), :] for at in at_rows]
        for i in parts[part]:
            at = pl.ds(i * PIECE, PIECE)
            mean = mean_ref[p, at, :]
            popped = [pltpu.matmul_pop(accs[x][i]) for x in range(2)]
            best = acc_ref[p, at, :]
            for n in range(CHUNK):
                piece = popped[n // 2][:, (n % 2) * LANES : (n % 2 + 1) * LANES]
                best = jnp.maximum(best, (piece - mean * totals[n]) * scales[n])
            acc_ref[p, at, :] = best

    def finish(p):
        spot = lax.broadcasted_iota(jnp.int32, (1, LANES), 1)
        limit = lengths_ref[p] - M
        for a in range(q_rows):
            if a < full:
                block = acc_ref[p, pl.ds(a * LANES, LANES), :]
                best = jnp.max(block.T, axis=0, keepdims=True)
            elif a == full:
                block = acc_ref[p, pl.ds(a * LANES, 8), :]
                best = jnp.broadcast_to(jnp.max(block, axis=1, keepdims=True)[:1], (1, LANES))
            if a <= full:
                best = best * q_scale_ref[pl.ds(p * q_pad + a, 1), :] * (1.0 / M)
                row = jnp.where(a * LANES + spot <= limit, 2.0 * (1.0 - best), 0.0)
            else:
                row = jnp.zeros((1, LANES), jnp.float32)
            out_ref[pl.ds(p, 1), pl.ds(a * LANES, LANES)] = row

    steps = per_device * chunks
    push(0)
    multiply(0, 0)
    multiply(0, 1)
    multiply(0, 2)
    push(1)
    fold(0, 0)

    @pl.loop(1, steps)
    def _(k):
        multiply(k, 0)
        fold(k - 1, 1)
        multiply(k, 1)
        fold(k - 1, 2)
        multiply(k, 2)
        push(lax.rem(k + 1, steps))
        fold(k, 0)

    fold(steps - 1, 1)
    fold(steps - 1, 2)
    for x in range(2):
        pltpu.matmul_acc_lhs(accs[x][0], left_ref[0, pl.ds(0, PIECE), :], load_staged_rhs=0)
        pltpu.matmul_pop(accs[x][0])
    for p in range(per_device):
        finish(p)
    copy(whole, 1).wait_send()


def join(members, groups, lengths, queries, block):
    per_device, series_len = queries.shape
    rows = block.shape[0]
    tall = (series_len - M) // LANES * LANES + PIECE
    q_rows = per_device * (series_len // LANES + 8)
    vmem = pl.BlockSpec(memory_space=pltpu.VMEM)
    return pl.pallas_call(
        functools.partial(join_kernel, members),
        out_shape=pltpu.VMEM((per_device, series_len), jnp.float32),
        in_specs=[pl.BlockSpec(memory_space=pl.ANY)] * 4,
        out_specs=vmem,
        scratch_shapes=[
            pltpu.VMEM((members + 1, rows, LANES), jnp.bfloat16),
            pltpu.VMEM((per_device, tall, M), jnp.bfloat16),
            pltpu.VMEM((per_device, tall, LANES), jnp.float32),
            pltpu.VMEM((per_device, rows + 24, LANES), jnp.float32),
            pltpu.VMEM((per_device, rows + PIECE, LANES), jnp.float32),
            pltpu.VMEM((per_device, rows + PIECE, LANES), jnp.float32),
            pltpu.VMEM((q_rows, LANES), jnp.float32),
            pltpu.VMEM((per_device, tall, LANES), jnp.float32),
            pltpu.VMEM((per_device, series_len), jnp.bfloat16),
            pltpu.SMEM((per_device,), jnp.int32),
            pltpu.SMEM((per_device,), jnp.int32),
            pltpu.SemaphoreType.DMA((4,)),
            pltpu.SemaphoreType.DMA((1,)),
            pltpu.SemaphoreType.DMA((1,)),
        ],
        compiler_params=pltpu.CompilerParams(collective_id=0, has_side_effects=True),
        name="join",
    )(groups, lengths, queries, block)


def body(long_series, queries, lengths, groups):
    members = lax.axis_size("ref")
    return join(members, groups, lengths, queries, long_series.reshape(-1, LANES))


def solution(mesh):
    in_specs = (
        P(("groups", "ref")),
        P(("groups", "ref"), None),
        P(("groups", "ref")),
        P(("groups", "ref")),
    )
    out_specs = P(("groups", "ref"), None)
    return jax.shard_map(body, mesh=mesh, in_specs=in_specs, out_specs=out_specs, check_vma=False)
```

```python
import functools

import jax
import jax.numpy as jnp
from jax import lax
from jax.experimental import pallas as pl
from jax.experimental.pallas import tpu as pltpu
from jax.sharding import PartitionSpec as P

M = 256
LANES = 128
WIDE = 2 * LANES
SPREAD_FLOOR = 0.25
CHUNK = 4
PIECE = 16
MASKED = -1e30


def iotas(shape):
    return (
        lax.broadcasted_iota(jnp.int32, shape, 0),
        lax.broadcasted_iota(jnp.int32, shape, 1),
    )


def hankel_tiles(rows):
    shape = (LANES, LANES)
    sub, lane = iotas(shape)
    rolled = [
        pltpu.roll(
            jnp.broadcast_to(row, shape).astype(jnp.bfloat16), 1, 1, stride=1, stride_axis=0
        )
        for row in rows
    ]
    return [
        jnp.where(lane <= sub, here, there) for here, there in zip(rolled, rolled[1:])
    ]


def toeplitz(row, following):
    shape = (LANES, LANES)
    sub, lane = iotas(shape)
    here = pltpu.roll(jnp.broadcast_to(row, shape), 0, 1, stride=1, stride_axis=0)
    there = pltpu.roll(jnp.broadcast_to(following, shape), 0, 1, stride=1, stride_axis=0)
    return jnp.where(lane >= sub, here, there)


def next_row(x):
    return pltpu.roll(x, x.shape[0] - 1, 0)


def window_scale(x):
    lane = lax.broadcasted_iota(jnp.int32, x.shape, 1)
    total, square = x, jnp.zeros_like(x)
    count = 1
    while count < M:
        def ahead(v):
            if count == LANES:
                return next_row(v)
            rolled = pltpu.roll(v, LANES - count, 1)
            return jnp.where(lane < LANES - count, rolled, next_row(rolled))

        total_ahead, square_ahead = ahead(total), ahead(square)
        gap = total - total_ahead
        square = square + square_ahead + gap * gap * (0.5 / count)
        total = total + total_ahead
        count *= 2
    return 1.0 / jnp.sqrt(square * (1.0 / M) + SPREAD_FLOOR)


def join_kernel(members, groups_hbm, lengths_hbm, q_hbm, block_hbm, out_ref,
                series_ref, left_ref, mean_ref, points_ref, total_ref, scale_ref,
                q_scale_ref, acc_ref, q_ref, groups_ref, lengths_ref,
                local_sem, send_sem, recv_sem):
    tall = left_ref.shape[1]
    pieces = tall // PIECE
    specs = [pltpu.ACC(x)((PIECE, WIDE), jnp.float32) for x in range(2) for _ in range(pieces)]

    def main(*accs):
        join_body(members, groups_hbm, lengths_hbm, q_hbm, block_hbm, out_ref,
                  series_ref, left_ref, mean_ref, points_ref, total_ref, scale_ref,
                  q_scale_ref, acc_ref, q_ref, groups_ref, lengths_ref,
                  local_sem, send_sem, recv_sem, (accs[:pieces], accs[pieces:]))

    pl.run_scoped(main, *specs)


def join_body(members, groups_hbm, lengths_hbm, q_hbm, block_hbm, out_ref,
              series_ref, left_ref, mean_ref, points_ref, total_ref, scale_ref,
              q_scale_ref, acc_ref, q_ref, groups_ref, lengths_ref,
              local_sem, send_sem, recv_sem, accs):
    per_device, series_len = q_ref.shape
    q_rows = series_len // LANES
    rows = block_hbm.shape[0]
    full = (series_len - M) // LANES
    tall = left_ref.shape[1]
    pieces = tall // PIECE
    q_pad = q_rows + 8
    chunks = rows // CHUNK
    me = lax.axis_index("ref")

    def place(d):
        return lax.rem(me + d, members)

    def slot(owner):
        return series_ref.at[owner]

    def copy(src, d):
        return pltpu.make_async_remote_copy(
            src_ref=src, dst_ref=src, send_sem=send_sem.at[0], recv_sem=recv_sem.at[0],
            device_id={"ref": place(d)}, device_id_type=pl.DeviceIdType.MESH,
        )

    fetches = [
        pltpu.make_async_copy(block_hbm, slot(me), local_sem.at[0]),
        pltpu.make_async_copy(q_hbm, q_ref, local_sem.at[1]),
        pltpu.make_async_copy(groups_hbm, groups_ref, local_sem.at[2]),
        pltpu.make_async_copy(lengths_hbm, lengths_ref, local_sem.at[3]),
    ]
    barrier = pltpu.get_barrier_semaphore()
    for fetch in fetches:
        fetch.start()

    @pl.loop(1, members)
    def _(d):
        pl.semaphore_signal(
            barrier, inc=1, device_id={"ref": place(d)}, device_id_type=pl.DeviceIdType.MESH
        )

    series_ref[members] = jnp.zeros((rows, LANES), jnp.bfloat16)
    acc_ref[...] = jnp.full(acc_ref.shape, MASKED, jnp.float32)
    fetches[0].wait()
    pl.semaphore_wait(barrier, members - 1)

    @pl.loop(1, members)
    def _(d):
        copy(slot(me), d).start()

    fetches[1].wait()
    fetches[2].wait()
    fetches[3].wait()

    sub, lane = iotas((WIDE, WIDE))
    flip = jnp.where(sub + lane == LANES - 1, 1.0, 0.0).astype(jnp.bfloat16)
    ones = jnp.full((WIDE, WIDE), 1.0 / M, jnp.bfloat16)
    q_all = q_ref[...].astype(jnp.float32)
    parts = []
    for p in range(per_device):
        row_list = [q_all[p : p + 1, LANES * a : LANES * (a + 1)] for a in range(q_rows)]
        parts += row_list + [jnp.zeros((q_pad - q_rows, LANES), jnp.float32)]
    q_points = jnp.concatenate(parts, axis=0)
    q_scale_ref[...] = window_scale(q_points)
    q_lhs = jnp.concatenate([q_points, jnp.zeros_like(q_points)], axis=1).astype(jnp.bfloat16)
    pltpu.matmul_push_rhs(flip, 0, 0)
    for p in range(per_device):
        pltpu.matmul_acc_lhs(
            accs[0][p], q_lhs[p * q_pad : (p + 1) * q_pad], load_staged_rhs=None if p else 0
        )
    for x in range(2):
        pltpu.matmul_push_rhs(ones, 0, x)
    for p in range(per_device):
        q_back = pltpu.matmul_pop(accs[0][p])[:, :LANES]
        for a in range(full + 2):
            tile = toeplitz(q_back[a : a + 1], q_back[a + 1 : a + 2]).astype(jnp.bfloat16)
            for h in range(2):
                if 0 <= a - h < full:
                    left_ref[p, pl.ds((a - h) * LANES, LANES), pl.ds(h * LANES, LANES)] = tile
                elif a - h == full:
                    left_ref[p, pl.ds(full * LANES, PIECE), pl.ds(h * LANES, LANES)] = tile[:PIECE]
    for p in range(per_device):
        for i in range(pieces):
            x = i % 2
            pltpu.matmul_acc_lhs(
                accs[x][i], left_ref[p, pl.ds(i * PIECE, PIECE), :],
                load_staged_rhs=0 if p == 0 and i < 2 else None,
            )
        for i in range(pieces):
            mean_ref[p, pl.ds(i * PIECE, PIECE), :] = pltpu.matmul_pop(accs[i % 2][i])[:, :LANES]

    near = jnp.where((lane >= LANES) | (sub >= LANES) | (sub >= lane), 1.0, 0.0).astype(jnp.bfloat16)
    far = jnp.where((sub < LANES) & (sub < lane), 1.0, 0.0).astype(jnp.bfloat16)
    for x in range(2):
        pltpu.matmul_push_rhs(near, 0, x)
        pltpu.matmul_push_rhs(far, 1, x)

    whole = series_ref.at[pl.ds(0, members - 1)]
    copy(whole, 1).wait_recv()

    for p in range(per_device):
        g = groups_ref[p]
        block = series_ref[g].astype(jnp.float32)
        ahead = series_ref[g + 1].astype(jnp.float32)
        points_ref[p, pl.ds(0, rows), :] = block
        points_ref[p, pl.ds(rows, 8), :] = ahead[:8]
        shape = (8, LANES)
        spot = lax.broadcasted_iota(jnp.int32, shape, 1)
        tail = jnp.concatenate([block[rows - 2 :], ahead[:6]], axis=0)
        moved = pltpu.roll(block[rows - 8 :], LANES - 1, 1)
        moved = jnp.where(spot < LANES - 1, moved, next_row(moved))
        moved = jnp.concatenate([moved[4:], moved[:4]], axis=0)
        final = jnp.full(shape, g, jnp.int32) == members - 1
        points_ref[p, pl.ds(rows + 8, 8), :] = jnp.where(final, moved, tail)
    for p in range(per_device):
        x = p % 2
        here, ahead, beyond = (points_ref[p, pl.ds(s, rows + PIECE), :] for s in range(3))

        def operand(f):
            close = jnp.concatenate([f(here), f(ahead)], axis=1)
            away = jnp.concatenate([f(beyond), jnp.zeros_like(f(beyond))], axis=1)
            return close, away

        def high(v):
            return (v * v).astype(jnp.bfloat16)

        def low(v):
            return (v * v - high(v).astype(jnp.float32)).astype(jnp.bfloat16)

        plain = operand(lambda v: v.astype(jnp.bfloat16))
        squares = [operand(high), operand(low)]
        stat_pieces = rows // PIECE + 1
        for s in range(2):
            for t in range(stat_pieces):
                cut = slice(t * PIECE, (t + 1) * PIECE)
                pltpu.matmul_acc_lhs(
                    accs[x][2 * t], plain[s][cut], load_staged_rhs=s if t == 0 else None
                )
                for square in squares:
                    pltpu.matmul_acc_lhs(accs[x][2 * t + 1], square[s][cut])
        for t in range(stat_pieces):
            total = pltpu.matmul_pop(accs[x][2 * t])[:, :LANES]
            square = pltpu.matmul_pop(accs[x][2 * t + 1])[:, :LANES]
            mean = total * (1.0 / M)
            spread = jnp.maximum(square * (1.0 / M) - mean * mean, 0.0)
            total_ref[p, pl.ds(t * PIECE, PIECE), :] = total
            scale_ref[p, pl.ds(t * PIECE, PIECE), :] = 1.0 / jnp.sqrt(spread + SPREAD_FLOOR)

    half = rows // 2

    def starts(c):
        return 2 * c, jnp.where(c == chunks - 1, rows + 8, half + 2 * c)

    def push(p, c):
        ends = c == chunks
        p = jnp.where(ends, lax.rem(p + 1, per_device), p)
        for x, first in enumerate(starts(jnp.where(ends, 0, c))):
            tiles = hankel_tiles([points_ref[p, pl.ds(first + m, 1), :] for m in range(4)])
            rhs = jnp.concatenate(
                [
                    jnp.concatenate([tiles[0], tiles[1]], axis=1),
                    jnp.concatenate([tiles[1], tiles[2]], axis=1),
                ],
                axis=0,
            )
            pltpu.matmul_push_rhs(rhs, 0, x)

    third = -(-pieces // 3)
    parts = [range(s, min(s + third, pieces)) for s in range(0, pieces, third)]

    def multiply(p, part):
        for i in parts[part]:
            lhs = left_ref[p, pl.ds(i * PIECE, PIECE), :]
            for x in range(2):
                pltpu.matmul_acc_lhs(accs[x][i], lhs, load_staged_rhs=None if i else 0)

    def fold(p, c, part):
        at_rows = [first + n for first in starts(c) for n in range(2)]
        totals = [total_ref[p, pl.ds(at, 1), :] for at in at_rows]
        scales = [scale_ref[p, pl.ds(at, 1), :] for at in at_rows]
        for i in parts[part]:
            at = pl.ds(i * PIECE, PIECE)
            mean = mean_ref[p, at, :]
            popped = [pltpu.matmul_pop(accs[x][i]) for x in range(2)]
            best = acc_ref[p, at, :]
            for n in range(CHUNK):
                piece = popped[n // 2][:, (n % 2) * LANES : (n % 2 + 1) * LANES]
                best = jnp.maximum(best, (piece - mean * totals[n]) * scales[n])
            acc_ref[p, at, :] = best

    def finish(p):
        spot = lax.broadcasted_iota(jnp.int32, (1, LANES), 1)
        limit = lengths_ref[p] - M
        for a in range(q_rows):
            if a < full:
                block = acc_ref[p, pl.ds(a * LANES, LANES), :]
                best = jnp.max(block.T, axis=0, keepdims=True)
            elif a == full:
                block = acc_ref[p, pl.ds(a * LANES, 8), :]
                best = jnp.broadcast_to(jnp.max(block, axis=1, keepdims=True)[:1], (1, LANES))
            if a <= full:
                best = best * q_scale_ref[pl.ds(p * q_pad + a, 1), :] * (1.0 / M)
                row = jnp.where(a * LANES + spot <= limit, 2.0 * (1.0 - best), 0.0)
            else:
                row = jnp.zeros((1, LANES), jnp.float32)
            out_ref[pl.ds(p, 1), pl.ds(a * LANES, LANES)] = row

    push(0, 0)
    for p in range(per_device):
        before = (p - 1, chunks - 1)
        multiply(p, 0)
        if p:
            fold(*before, 1)
        multiply(p, 1)
        if p:
            fold(*before, 2)
        multiply(p, 2)
        push(p, 1)
        fold(p, 0, 0)
        if p:
            finish(p - 1)

        @pl.loop(1, chunks)
        def _(c):
            multiply(p, 0)
            fold(p, c - 1, 1)
            multiply(p, 1)
            fold(p, c - 1, 2)
            multiply(p, 2)
            push(p, c + 1)
            fold(p, c, 0)

    fold(per_device - 1, chunks - 1, 1)
    fold(per_device - 1, chunks - 1, 2)
    for x in range(2):
        pltpu.matmul_acc_lhs(accs[x][0], left_ref[0, pl.ds(0, PIECE), :], load_staged_rhs=0)
        pltpu.matmul_pop(accs[x][0])
    finish(per_device - 1)
    copy(whole, 1).wait_send()


def join(members, groups, lengths, queries, block):
    per_device, series_len = queries.shape
    rows = block.shape[0]
    tall = (series_len - M) // LANES * LANES + PIECE
    q_rows = per_device * (series_len // LANES + 8)
    vmem = pl.BlockSpec(memory_space=pltpu.VMEM)
    return pl.pallas_call(
        functools.partial(join_kernel, members),
        out_shape=pltpu.VMEM((per_device, series_len), jnp.float32),
        in_specs=[pl.BlockSpec(memory_space=pl.ANY)] * 4,
        out_specs=vmem,
        scratch_shapes=[
            pltpu.VMEM((members + 1, rows, LANES), jnp.bfloat16),
            pltpu.VMEM((per_device, tall, M), jnp.bfloat16),
            pltpu.VMEM((per_device, tall, LANES), jnp.float32),
            pltpu.VMEM((per_device, rows + 24, LANES), jnp.float32),
            pltpu.VMEM((per_device, rows + PIECE, LANES), jnp.float32),
            pltpu.VMEM((per_device, rows + PIECE, LANES), jnp.float32),
            pltpu.VMEM((q_rows, LANES), jnp.float32),
            pltpu.VMEM((per_device, tall, LANES), jnp.float32),
            pltpu.VMEM((per_device, series_len), jnp.bfloat16),
            pltpu.SMEM((per_device,), jnp.int32),
            pltpu.SMEM((per_device,), jnp.int32),
            pltpu.SemaphoreType.DMA((4,)),
            pltpu.SemaphoreType.DMA((1,)),
            pltpu.SemaphoreType.DMA((1,)),
        ],
        compiler_params=pltpu.CompilerParams(collective_id=0, has_side_effects=True),
        name="join",
    )(groups, lengths, queries, block)


def body(long_series, queries, lengths, groups):
    members = lax.axis_size("ref")
    return join(members, groups, lengths, queries, long_series.reshape(-1, LANES))


def solution(mesh):
    in_specs = (
        P(("groups", "ref")),
        P(("groups", "ref"), None),
        P(("groups", "ref")),
        P(("groups", "ref")),
    )
    out_specs = P(("groups", "ref"), None)
    return jax.shard_map(body, mesh=mesh, in_specs=in_specs, out_specs=out_specs, check_vma=False)
```

```python
import functools

import jax
import jax.numpy as jnp
from jax import lax
from jax.experimental import pallas as pl
from jax.experimental.pallas import tpu as pltpu
from jax.sharding import PartitionSpec as P

M = 256
LANES = 128
WIDE = 2 * LANES
SPREAD_FLOOR = 0.25
CHUNK = 4
PIECE = 16
SHORT = 17
LAG = 28
LEVELS = 3
MASKED = -1e30


def iotas(shape):
    return (
        lax.broadcasted_iota(jnp.int32, shape, 0),
        lax.broadcasted_iota(jnp.int32, shape, 1),
    )


def hankel_tiles(rows):
    shape = (LANES, LANES)
    sub, lane = iotas(shape)
    rolled = [
        pltpu.roll(
            jnp.broadcast_to(row, shape).astype(jnp.bfloat16), 1, 1, stride=1, stride_axis=0
        )
        for row in rows
    ]
    return [
        jnp.where(lane <= sub, here, there) for here, there in zip(rolled, rolled[1:])
    ]


def toeplitz(row, following):
    shape = (LANES, LANES)
    sub, lane = iotas(shape)
    here = pltpu.roll(jnp.broadcast_to(row, shape), 0, 1, stride=1, stride_axis=0)
    there = pltpu.roll(jnp.broadcast_to(following, shape), 0, 1, stride=1, stride_axis=0)
    return jnp.where(lane >= sub, here, there)


def next_row(x):
    return pltpu.roll(x, x.shape[0] - 1, 0)


def window_scale(x):
    lane = lax.broadcasted_iota(jnp.int32, x.shape, 1)
    total, square = x, jnp.zeros_like(x)
    count = 1
    while count < M:
        def ahead(v):
            if count == LANES:
                return next_row(v)
            rolled = pltpu.roll(v, LANES - count, 1)
            return jnp.where(lane < LANES - count, rolled, next_row(rolled))

        total_ahead, square_ahead = ahead(total), ahead(square)
        gap = total - total_ahead
        square = square + square_ahead + gap * gap * (0.5 / count)
        total = total + total_ahead
        count *= 2
    return 1.0 / jnp.sqrt(square * (1.0 / M) + SPREAD_FLOOR)


def gather_kernel(members, groups_hbm, lengths_hbm, q_hbm, block_hbm,
                  series_ref, left_ref, mean_ref, q_scale_ref, band_ref, groups_ref, lengths_ref,
                  q_ref, local_sem, send_sem, recv_sem):
    pieces = left_ref.shape[0] // lengths_ref.shape[0] // PIECE
    specs = [pltpu.ACC(x)((PIECE, WIDE), jnp.float32) for x in range(2) for _ in range(pieces)]

    def main(*accs):
        gather_body(members, groups_hbm, lengths_hbm, q_hbm, block_hbm,
                    series_ref, left_ref, mean_ref, q_scale_ref, band_ref, groups_ref, lengths_ref,
                    q_ref, local_sem, send_sem, recv_sem, (accs[:pieces], accs[pieces:]))

    pl.run_scoped(main, *specs)


def gather_body(members, groups_hbm, lengths_hbm, q_hbm, block_hbm,
                series_ref, left_ref, mean_ref, q_scale_ref, band_ref, groups_ref, lengths_ref,
                q_ref, local_sem, send_sem, recv_sem, accs):
    per_device, series_len = q_ref.shape
    q_rows = series_len // LANES
    rows = block_hbm.shape[0]
    full = (series_len - M) // LANES
    tall = left_ref.shape[0] // per_device
    pieces = tall // PIECE
    q_pad = q_rows + 8
    me = lax.axis_index("ref")

    def place(d):
        return lax.rem(me + d, members)

    def copy(src, d):
        return pltpu.make_async_remote_copy(
            src_ref=src, dst_ref=src, send_sem=send_sem.at[0], recv_sem=recv_sem.at[0],
            device_id={"ref": place(d)}, device_id_type=pl.DeviceIdType.MESH,
        )

    fetches = [
        pltpu.make_async_copy(block_hbm, series_ref.at[me], local_sem.at[0]),
        pltpu.make_async_copy(q_hbm, q_ref, local_sem.at[1]),
        pltpu.make_async_copy(groups_hbm, groups_ref, local_sem.at[2]),
        pltpu.make_async_copy(lengths_hbm, lengths_ref, local_sem.at[3]),
    ]
    barrier = pltpu.get_barrier_semaphore()
    for fetch in fetches:
        fetch.start()

    @pl.loop(1, members)
    def _(d):
        pl.semaphore_signal(
            barrier, inc=1, device_id={"ref": place(d)}, device_id_type=pl.DeviceIdType.MESH
        )

    series_ref[members] = jnp.zeros((rows, LANES), jnp.bfloat16)
    fetches[0].wait()
    pl.semaphore_wait(barrier, members - 1)

    @pl.loop(1, members)
    def _(d):
        copy(series_ref.at[me], d).start()

    fetches[1].wait()
    fetches[2].wait()
    fetches[3].wait()

    sub, lane = iotas((WIDE, WIDE))
    flip = jnp.where(sub + lane == LANES - 1, 1.0, 0.0).astype(jnp.bfloat16)
    ones = jnp.full((WIDE, WIDE), 1.0 / M, jnp.bfloat16)
    q_all = q_ref[...].astype(jnp.float32)
    parts = []
    for p in range(per_device):
        row_list = [q_all[p : p + 1, LANES * a : LANES * (a + 1)] for a in range(q_rows)]
        parts += row_list + [jnp.zeros((q_pad - q_rows, LANES), jnp.float32)]
    q_points = jnp.concatenate(parts, axis=0)
    q_scale_ref[...] = window_scale(q_points)
    q_lhs = jnp.concatenate([q_points, jnp.zeros_like(q_points)], axis=1).astype(jnp.bfloat16)
    pltpu.matmul_push_rhs(flip, 0, 0)
    for p in range(per_device):
        pltpu.matmul_acc_lhs(
            accs[0][p], q_lhs[p * q_pad : (p + 1) * q_pad], load_staged_rhs=None if p else 0
        )
    for x in range(2):
        pltpu.matmul_push_rhs(ones, 0, x)
    for p in range(per_device):
        q_back = pltpu.matmul_pop(accs[0][p])[:, :LANES]
        for a in range(full + 2):
            tile = toeplitz(q_back[a : a + 1], q_back[a + 1 : a + 2]).astype(jnp.bfloat16)
            for h in range(2):
                if 0 <= a - h < full:
                    left_ref[pl.ds(p * tall + (a - h) * LANES, LANES), pl.ds(h * LANES, LANES)] = tile
                elif a - h == full:
                    left_ref[pl.ds(p * tall + full * LANES, PIECE), pl.ds(h * LANES, LANES)] = tile[:PIECE]
    for p in range(per_device):
        for i in range(pieces):
            x = i % 2
            pltpu.matmul_acc_lhs(
                accs[x][i], left_ref[pl.ds(p * tall + i * PIECE, PIECE), :],
                load_staged_rhs=0 if p == 0 and i < 2 else None,
            )
        for i in range(pieces):
            mean_ref[pl.ds(p * tall + i * PIECE, PIECE), :] = pltpu.matmul_pop(accs[i % 2][i])[:, :LANES]

    band_ref[0] = jnp.where(
        (lane >= LANES) | (sub >= LANES) | (sub >= lane), 1.0, 0.0
    ).astype(jnp.bfloat16)
    band_ref[1] = jnp.where((sub < LANES) & (sub < lane), 1.0, 0.0).astype(jnp.bfloat16)

    whole = series_ref.at[pl.ds(0, members - 1)]
    copy(whole, 1).wait_recv()
    copy(whole, 1).wait_send()


def join_kernel(series_ref, left_ref, mean_ref, q_scale_ref, band_ref, groups_ref, lengths_ref,
                out_ref, points_ref, total_ref, scale_ref, acc_ref, rows_ref):
    slots = 60
    specs = [pltpu.ACC(x)((PIECE, WIDE), jnp.float32) for x in range(2) for _ in range(slots)]

    def main(*accs):
        join_body(series_ref, left_ref, mean_ref, q_scale_ref, band_ref, groups_ref, lengths_ref,
                  out_ref, points_ref, total_ref, scale_ref, acc_ref, rows_ref,
                  (accs[:slots], accs[slots:]))

    pl.run_scoped(main, *specs)


def join_body(series_ref, left_ref, mean_ref, q_scale_ref, band_ref, groups_ref, lengths_ref,
              out_ref, points_ref, total_ref, scale_ref, acc_ref, rows_ref, accs):
    per_device, series_len = out_ref.shape
    members, rows = series_ref.shape[0] - 1, series_ref.shape[1]
    q_rows = series_len // LANES
    q_pad = q_rows + 8
    full = (series_len - M) // LANES
    tall = left_ref.shape[0] // per_device
    chunks = rows // CHUNK
    half = rows // 2

    for x in range(2):
        for r in range(2):
            pltpu.matmul_push_rhs(band_ref[r], r, x)

    for p in range(per_device):
        g = groups_ref[p]
        block = series_ref[g].astype(jnp.float32)
        ahead = series_ref[g + 1].astype(jnp.float32)
        points_ref[p, pl.ds(0, rows), :] = block
        points_ref[p, pl.ds(rows, 8), :] = ahead[:8]
        shape = (8, LANES)
        spot = lax.broadcasted_iota(jnp.int32, shape, 1)
        tail = jnp.concatenate([block[rows - 2 :], ahead[:6]], axis=0)
        moved = pltpu.roll(block[rows - 8 :], LANES - 1, 1)
        moved = jnp.where(spot < LANES - 1, moved, next_row(moved))
        moved = jnp.concatenate([moved[4:], moved[:4]], axis=0)
        final = jnp.full(shape, g, jnp.int32) == members - 1
        points_ref[p, pl.ds(rows + 8, 8), :] = jnp.where(final, moved, tail)
        points_ref[p, pl.ds(rows + 16, 8), :] = jnp.zeros(shape, jnp.float32)
    for p in range(per_device):
        x = p % 2
        here, ahead, beyond = (points_ref[p, pl.ds(s, rows + PIECE), :] for s in range(3))

        def operand(f):
            close = jnp.concatenate([f(here), f(ahead)], axis=1)
            away = jnp.concatenate([f(beyond), jnp.zeros_like(f(beyond))], axis=1)
            return close, away

        def high(v):
            return (v * v).astype(jnp.bfloat16)

        def low(v):
            return (v * v - high(v).astype(jnp.float32)).astype(jnp.bfloat16)

        plain = operand(lambda v: v.astype(jnp.bfloat16))
        squares = [operand(high), operand(low)]
        stat_pieces = rows // PIECE + 1
        for s in range(2):
            for t in range(stat_pieces):
                cut = slice(t * PIECE, (t + 1) * PIECE)
                pltpu.matmul_acc_lhs(
                    accs[x][2 * t], plain[s][cut], load_staged_rhs=s if t == 0 else None
                )
                for square in squares:
                    pltpu.matmul_acc_lhs(accs[x][2 * t + 1], square[s][cut])
        for t in range(stat_pieces):
            total = pltpu.matmul_pop(accs[x][2 * t])[:, :LANES]
            square = pltpu.matmul_pop(accs[x][2 * t + 1])[:, :LANES]
            mean = total * (1.0 / M)
            spread = jnp.maximum(square * (1.0 / M) - mean * mean, 0.0)
            total_ref[p, pl.ds(t * PIECE, PIECE), :] = total
            scale_ref[p, pl.ds(t * PIECE, PIECE), :] = 1.0 / jnp.sqrt(spread + SPREAD_FLOOR)

    def starts(c):
        if isinstance(c, int):
            return 2 * c, rows + 8 if c == chunks - 1 else half + 2 * c
        return 2 * c, jnp.where(c == chunks - 1, rows + 8, half + 2 * c)

    def push(p, c, register):
        for x, first in enumerate(starts(c)):
            tiles = hankel_tiles([points_ref[p, pl.ds(first + m, 1), :] for m in range(4)])
            rhs = jnp.concatenate(
                [
                    jnp.concatenate([tiles[0], tiles[1]], axis=1),
                    jnp.concatenate([tiles[1], tiles[2]], axis=1),
                ],
                axis=0,
            )
            pltpu.matmul_push_rhs(rhs, register, x)

    def finish(blocks, p):
        spot = lax.broadcasted_iota(jnp.int32, (1, LANES), 1)
        limit = lengths_ref[p] - M
        for a in range(blocks + 1):
            if a < blocks:
                block = acc_ref[pl.ds(a * LANES, LANES), :]
                best = jnp.max(block.T, axis=0, keepdims=True)
            else:
                block = acc_ref[pl.ds(a * LANES, 8), :]
                best = jnp.broadcast_to(jnp.max(block, axis=1, keepdims=True)[:1], (1, LANES))
            best = best * q_scale_ref[pl.ds(p * q_pad + a, 1), :] * (1.0 / M)
            row = jnp.where(a * LANES + spot <= limit, 2.0 * (1.0 - best), 0.0)
            rows_ref[pl.ds(p * q_rows + a, 1), :] = row

    def row(p, j):
        return pl.ds(pl.multiple_of(p * tall, PIECE) + j * PIECE, PIECE)

    def multiply(p, j, slot, register):
        lhs = left_ref[row(p, j), :]
        for x in range(2):
            pltpu.matmul_acc_lhs(accs[x][slot], lhs, load_staged_rhs=register)

    def weights(p, c):
        at = [first + n for first in starts(c) for n in range(2)]
        return [[ref[p, pl.ds(r, 1), :] for r in at] for ref in (total_ref, scale_ref)]

    def fold(p, j, slot, totals, scales):
        mean = mean_ref[row(p, j), :]
        popped = [pltpu.matmul_pop(accs[x][slot]) for x in range(2)]
        at = pl.ds(j * PIECE, PIECE)
        best = acc_ref[at, :]
        for n in range(CHUNK):
            piece = popped[n // 2][:, (n % 2) * LANES : (n % 2 + 1) * LANES]
            best = jnp.maximum(best, (piece - mean * totals[n]) * scales[n])
        acc_ref[at, :] = best

    def pending(p, pieces, c, slots):
        known = []

        def one(s):
            if not known:
                known.append(weights(p, c))
            fold(p, s % pieces, s % slots, *known[0])

        return [functools.partial(one, s) for s in range(pieces)]

    def begin(pieces):
        rest = pl.ds(0, pieces * PIECE)
        acc_ref[rest, :] = jnp.full((pieces * PIECE, LANES), MASKED, jnp.float32)

    def visit_short(pieces, p, then, todo, close):
        total = chunks * pieces
        slots = len(accs[0]) // pieces * pieces
        known = {}

        def one(s):
            c = s // pieces
            if c not in known:
                known[c] = weights(p, c)
            fold(p, s % pieces, s % slots, *known[c])

        ours = [functools.partial(one, s) for s in range(total)]
        lag = len(todo) or LAG
        for s in range(total):
            c, j = s // pieces, s % pieces
            multiply(p, j, s % slots, None if j else c % 2)
            if s == 0:
                push(p, 1, 1)
            if j == 0 and c + 2 < chunks:
                push(p, c + 2, c % 2)
            if j == 0 and c + 2 == chunks and then is not None:
                push(then, 0, 0)
            if s < len(todo):
                todo[s]()
            if s + 1 == lag:
                close()
                begin(pieces)
            if s >= lag:
                ours[s - lag]()
        return ours[total - lag :]

    def visit_long(pieces, p, then, todo, close):
        lag = min(LAG, pieces - 4)

        def pushes(c):
            if then is None:
                push(p, jnp.minimum(c, chunks - 1), 0)
            else:
                ends = c == chunks
                push(jnp.where(ends, then, p), jnp.where(ends, 0, c), 0)

        skip = len(todo) or lag
        ours = pending(p, pieces, 0, pieces)
        for s in range(pieces):
            multiply(p, s, s, None if s else 0)
            if s == 0:
                push(p, 1, 0)
            if s < len(todo):
                todo[s]()
            if s + 1 == skip:
                close()
                begin(pieces)
            if s >= skip:
                ours[s - skip]()
        for s in range(pieces - skip, pieces - lag):
            ours[s]()

        @pl.loop(1, chunks)
        def _(c):
            before, ours = pending(p, pieces, c - 1, pieces), pending(p, pieces, c, pieces)
            both = before[pieces - lag :] + ours
            for s in range(pieces):
                multiply(p, s, s, None if s else 0)
                if s == 0:
                    pushes(c + 1)
                both[s]()

        return pending(p, pieces, chunks - 1, pieces)[pieces - lag :]

    def run(sizes, order):
        todo, close = [], lambda: None
        for n, (blocks, p) in enumerate(zip(sizes, order)):
            then = order[n + 1] if n + 1 < len(order) else None
            pieces = blocks * (LANES // PIECE) + 1
            visit = visit_short if pieces <= SHORT else visit_long
            todo = visit(pieces, p, then, todo, close)
            close = functools.partial(finish, blocks, p)
        for step in todo:
            step()
        close()
        if pieces > SHORT:
            for x in range(2):
                pltpu.matmul_acc_lhs(accs[x][0], left_ref[pl.ds(0, PIECE), :], load_staged_rhs=0)
                pltpu.matmul_pop(accs[x][0])

    rows_ref[...] = jnp.zeros(rows_ref.shape, jnp.float32)
    levels = [full * (n + 1) // LEVELS for n in range(LEVELS)]
    blocks = [(lengths_ref[p] - M + LANES - 1) // LANES for p in range(per_device)]
    swap = blocks[1] > blocks[0]
    first, second = jnp.where(swap, 1, 0), jnp.where(swap, 0, 1)
    more, less = jnp.maximum(*blocks), jnp.minimum(*blocks)
    more, less = (
        sum((v > level).astype(jnp.int32) for level in levels[:-1]) for v in (more, less)
    )
    push(first, 0, 0)
    pairs = [(levels[m], levels[n]) for m in range(LEVELS) for n in range(m + 1)]
    lax.switch(
        more * (more + 1) // 2 + less,
        [functools.partial(run, pair) for pair in pairs],
        (first, second),
    )
    for p in range(per_device):
        for a in range(q_rows):
            out_ref[pl.ds(p, 1), pl.ds(a * LANES, LANES)] = rows_ref[pl.ds(p * q_rows + a, 1), :]


def join(members, groups, lengths, queries, block):
    per_device, series_len = queries.shape
    rows = block.shape[0]
    q_rows = series_len // LANES
    tall = (series_len - M) // LANES * LANES + PIECE
    vmem = pl.BlockSpec(memory_space=pltpu.VMEM)
    smem = pl.BlockSpec(memory_space=pltpu.SMEM)
    gathered = pl.pallas_call(
        functools.partial(gather_kernel, members),
        out_shape=(
            pltpu.VMEM((members + 1, rows, LANES), jnp.bfloat16),
            pltpu.VMEM((per_device * tall, M), jnp.bfloat16),
            pltpu.VMEM((per_device * tall, LANES), jnp.float32),
            pltpu.VMEM((per_device * (q_rows + 8), LANES), jnp.float32),
            pltpu.VMEM((2, WIDE, WIDE), jnp.bfloat16),
            pltpu.SMEM((per_device,), jnp.int32),
            pltpu.SMEM((per_device,), jnp.int32),
        ),
        in_specs=[pl.BlockSpec(memory_space=pl.ANY)] * 4,
        out_specs=(vmem,) * 5 + (smem,) * 2,
        scratch_shapes=[
            pltpu.VMEM((per_device, series_len), jnp.bfloat16),
            pltpu.SemaphoreType.DMA((4,)),
            pltpu.SemaphoreType.DMA((1,)),
            pltpu.SemaphoreType.DMA((1,)),
        ],
        compiler_params=pltpu.CompilerParams(
            collective_id=0, has_side_effects=True
        ),
        name="gather",
    )(groups, lengths, queries, block)
    spaces = (pltpu.VMEM,) * 5 + (pltpu.SMEM,) * 2
    held = [pltpu.with_memory_space_constraint(x, space) for x, space in zip(gathered, spaces)]
    return pl.pallas_call(
        join_kernel,
        out_shape=jax.ShapeDtypeStruct((per_device, series_len), jnp.float32),
        in_specs=[vmem] * 5 + [smem] * 2,
        out_specs=vmem,
        scratch_shapes=[
            pltpu.VMEM((per_device, rows + 24, LANES), jnp.float32),
            pltpu.VMEM((per_device, rows + PIECE, LANES), jnp.float32),
            pltpu.VMEM((per_device, rows + PIECE, LANES), jnp.float32),
            pltpu.VMEM((tall, LANES), jnp.float32),
            pltpu.VMEM((per_device * q_rows + 8, LANES), jnp.float32),
        ],
        compiler_params=pltpu.CompilerParams(

        ),
        name="join",
    )(*held)


def body(long_series, queries, lengths, groups):
    members = lax.axis_size("ref")
    return join(members, groups, lengths, queries, long_series.reshape(-1, LANES))


def solution(mesh):
    in_specs = (
        P(("groups", "ref")),
        P(("groups", "ref"), None),
        P(("groups", "ref")),
        P(("groups", "ref")),
    )
    out_specs = P(("groups", "ref"), None)
    return jax.shard_map(body, mesh=mesh, in_specs=in_specs, out_specs=out_specs, check_vma=False)
```

```python
import functools

import jax
import jax.numpy as jnp
from jax import lax
from jax.experimental import pallas as pl
from jax.experimental.pallas import tpu as pltpu
from jax.sharding import PartitionSpec as P

M = 256
LANES = 128
WIDE = 2 * LANES
SPREAD_FLOOR = 0.25
CHUNK = 4
PIECE = 16
SHORT = 17
LAG = 28
MASKED = -1e30


def iotas(shape):
    return (
        lax.broadcasted_iota(jnp.int32, shape, 0),
        lax.broadcasted_iota(jnp.int32, shape, 1),
    )


def hankel_tiles(rows):
    shape = (LANES, LANES)
    sub, lane = iotas(shape)
    rolled = [
        pltpu.roll(
            jnp.broadcast_to(row, shape).astype(jnp.bfloat16), 1, 1, stride=1, stride_axis=0
        )
        for row in rows
    ]
    return [
        jnp.where(lane <= sub, here, there) for here, there in zip(rolled, rolled[1:])
    ]


def toeplitz(row, following):
    shape = (LANES, LANES)
    sub, lane = iotas(shape)
    here = pltpu.roll(jnp.broadcast_to(row, shape), 0, 1, stride=1, stride_axis=0)
    there = pltpu.roll(jnp.broadcast_to(following, shape), 0, 1, stride=1, stride_axis=0)
    return jnp.where(lane >= sub, here, there)


def next_row(x):
    return pltpu.roll(x, x.shape[0] - 1, 0)


def window_scale(x):
    lane = lax.broadcasted_iota(jnp.int32, x.shape, 1)
    total, square = x, jnp.zeros_like(x)
    count = 1
    while count < M:
        def ahead(v):
            if count == LANES:
                return next_row(v)
            rolled = pltpu.roll(v, LANES - count, 1)
            return jnp.where(lane < LANES - count, rolled, next_row(rolled))

        total_ahead, square_ahead = ahead(total), ahead(square)
        gap = total - total_ahead
        square = square + square_ahead + gap * gap * (0.5 / count)
        total = total + total_ahead
        count *= 2
    return 1.0 / jnp.sqrt(square * (1.0 / M) + SPREAD_FLOOR)


def gather_kernel(members, groups_hbm, lengths_hbm, q_hbm, block_hbm,
                  series_ref, left_ref, mean_ref, q_scale_ref, band_ref, groups_ref, lengths_ref,
                  q_ref, local_sem, send_sem, recv_sem):
    pieces = left_ref.shape[0] // lengths_ref.shape[0] // PIECE
    specs = [pltpu.ACC(x)((PIECE, WIDE), jnp.float32) for x in range(2) for _ in range(pieces)]

    def main(*accs):
        gather_body(members, groups_hbm, lengths_hbm, q_hbm, block_hbm,
                    series_ref, left_ref, mean_ref, q_scale_ref, band_ref, groups_ref, lengths_ref,
                    q_ref, local_sem, send_sem, recv_sem, (accs[:pieces], accs[pieces:]))

    pl.run_scoped(main, *specs)


def gather_body(members, groups_hbm, lengths_hbm, q_hbm, block_hbm,
                series_ref, left_ref, mean_ref, q_scale_ref, band_ref, groups_ref, lengths_ref,
                q_ref, local_sem, send_sem, recv_sem, accs):
    per_device, series_len = q_ref.shape
    q_rows = series_len // LANES
    rows = block_hbm.shape[0]
    full = (series_len - M) // LANES
    tall = left_ref.shape[0] // per_device
    pieces = tall // PIECE
    q_pad = q_rows + 8
    me = lax.axis_index("ref")

    def place(d):
        return lax.rem(me + d, members)

    def copy(src, d):
        return pltpu.make_async_remote_copy(
            src_ref=src, dst_ref=src, send_sem=send_sem.at[0], recv_sem=recv_sem.at[0],
            device_id={"ref": place(d)}, device_id_type=pl.DeviceIdType.MESH,
        )

    fetches = [
        pltpu.make_async_copy(block_hbm, series_ref.at[me], local_sem.at[0]),
        pltpu.make_async_copy(q_hbm, q_ref, local_sem.at[1]),
        pltpu.make_async_copy(groups_hbm, groups_ref, local_sem.at[2]),
        pltpu.make_async_copy(lengths_hbm, lengths_ref, local_sem.at[3]),
    ]
    barrier = pltpu.get_barrier_semaphore()
    for fetch in fetches:
        fetch.start()

    @pl.loop(1, members)
    def _(d):
        pl.semaphore_signal(
            barrier, inc=1, device_id={"ref": place(d)}, device_id_type=pl.DeviceIdType.MESH
        )

    series_ref[members] = jnp.zeros((rows, LANES), jnp.bfloat16)
    fetches[0].wait()
    pl.semaphore_wait(barrier, members - 1)

    @pl.loop(1, members)
    def _(d):
        copy(series_ref.at[me], d).start()

    fetches[1].wait()
    fetches[2].wait()
    fetches[3].wait()

    sub, lane = iotas((WIDE, WIDE))
    flip = jnp.where(sub + lane == LANES - 1, 1.0, 0.0).astype(jnp.bfloat16)
    ones = jnp.full((WIDE, WIDE), 1.0 / M, jnp.bfloat16)
    q_all = q_ref[...].astype(jnp.float32)
    parts = []
    for p in range(per_device):
        row_list = [q_all[p : p + 1, LANES * a : LANES * (a + 1)] for a in range(q_rows)]
        parts += row_list + [jnp.zeros((q_pad - q_rows, LANES), jnp.float32)]
    q_points = jnp.concatenate(parts, axis=0)
    q_scale_ref[...] = window_scale(q_points)
    q_lhs = jnp.concatenate([q_points, jnp.zeros_like(q_points)], axis=1).astype(jnp.bfloat16)
    pltpu.matmul_push_rhs(flip, 0, 0)
    for p in range(per_device):
        pltpu.matmul_acc_lhs(
            accs[0][p], q_lhs[p * q_pad : (p + 1) * q_pad], load_staged_rhs=None if p else 0
        )
    for x in range(2):
        pltpu.matmul_push_rhs(ones, 0, x)
    for p in range(per_device):
        q_back = pltpu.matmul_pop(accs[0][p])[:, :LANES]
        for a in range(full + 2):
            tile = toeplitz(q_back[a : a + 1], q_back[a + 1 : a + 2]).astype(jnp.bfloat16)
            for h in range(2):
                if 0 <= a - h < full:
                    left_ref[pl.ds(p * tall + (a - h) * LANES, LANES), pl.ds(h * LANES, LANES)] = tile
                elif a - h == full:
                    left_ref[pl.ds(p * tall + full * LANES, PIECE), pl.ds(h * LANES, LANES)] = tile[:PIECE]
    for p in range(per_device):
        for i in range(pieces):
            x = i % 2
            pltpu.matmul_acc_lhs(
                accs[x][i], left_ref[pl.ds(p * tall + i * PIECE, PIECE), :],
                load_staged_rhs=0 if p == 0 and i < 2 else None,
            )
        for i in range(pieces):
            mean_ref[pl.ds(p * tall + i * PIECE, PIECE), :] = pltpu.matmul_pop(accs[i % 2][i])[:, :LANES]

    band_ref[0] = jnp.where(
        (lane >= LANES) | (sub >= LANES) | (sub >= lane), 1.0, 0.0
    ).astype(jnp.bfloat16)
    band_ref[1] = jnp.where((sub < LANES) & (sub < lane), 1.0, 0.0).astype(jnp.bfloat16)

    whole = series_ref.at[pl.ds(0, members - 1)]
    copy(whole, 1).wait_recv()
    copy(whole, 1).wait_send()


def join_kernel(series_ref, left_ref, mean_ref, q_scale_ref, band_ref, groups_ref, lengths_ref,
                out_ref, points_ref, total_ref, scale_ref, acc_ref, rows_ref):
    slots = 60
    specs = [pltpu.ACC(x)((PIECE, WIDE), jnp.float32) for x in range(2) for _ in range(slots)]

    def main(*accs):
        join_body(series_ref, left_ref, mean_ref, q_scale_ref, band_ref, groups_ref, lengths_ref,
                  out_ref, points_ref, total_ref, scale_ref, acc_ref, rows_ref,
                  (accs[:slots], accs[slots:]))

    pl.run_scoped(main, *specs)


def join_body(series_ref, left_ref, mean_ref, q_scale_ref, band_ref, groups_ref, lengths_ref,
              out_ref, points_ref, total_ref, scale_ref, acc_ref, rows_ref, accs):
    per_device, series_len = out_ref.shape
    members, rows = series_ref.shape[0] - 1, series_ref.shape[1]
    q_rows = series_len // LANES
    q_pad = q_rows + 8
    full = (series_len - M) // LANES
    tall = left_ref.shape[0] // per_device
    chunks = rows // CHUNK
    half = rows // 2

    for x in range(2):
        for r in range(2):
            pltpu.matmul_push_rhs(band_ref[r], r, x)

    for p in range(per_device):
        g = groups_ref[p]
        block = series_ref[g].astype(jnp.float32)
        ahead = series_ref[g + 1].astype(jnp.float32)
        points_ref[p, pl.ds(0, rows), :] = block
        points_ref[p, pl.ds(rows, 8), :] = ahead[:8]
        shape = (8, LANES)
        spot = lax.broadcasted_iota(jnp.int32, shape, 1)
        tail = jnp.concatenate([block[rows - 2 :], ahead[:6]], axis=0)
        moved = pltpu.roll(block[rows - 8 :], LANES - 1, 1)
        moved = jnp.where(spot < LANES - 1, moved, next_row(moved))
        moved = jnp.concatenate([moved[4:], moved[:4]], axis=0)
        final = jnp.full(shape, g, jnp.int32) == members - 1
        points_ref[p, pl.ds(rows + 8, 8), :] = jnp.where(final, moved, tail)
        points_ref[p, pl.ds(rows + 16, 8), :] = jnp.zeros(shape, jnp.float32)
    for p in range(per_device):
        x = p % 2
        here, ahead, beyond = (points_ref[p, pl.ds(s, rows + PIECE), :] for s in range(3))

        def operand(f):
            close = jnp.concatenate([f(here), f(ahead)], axis=1)
            away = jnp.concatenate([f(beyond), jnp.zeros_like(f(beyond))], axis=1)
            return close, away

        def high(v):
            return (v * v).astype(jnp.bfloat16)

        def low(v):
            return (v * v - high(v).astype(jnp.float32)).astype(jnp.bfloat16)

        plain = operand(lambda v: v.astype(jnp.bfloat16))
        squares = [operand(high), operand(low)]
        stat_pieces = rows // PIECE + 1
        for s in range(2):
            for t in range(stat_pieces):
                cut = slice(t * PIECE, (t + 1) * PIECE)
                pltpu.matmul_acc_lhs(
                    accs[x][2 * t], plain[s][cut], load_staged_rhs=s if t == 0 else None
                )
                for square in squares:
                    pltpu.matmul_acc_lhs(accs[x][2 * t + 1], square[s][cut])
        for t in range(stat_pieces):
            total = pltpu.matmul_pop(accs[x][2 * t])[:, :LANES]
            square = pltpu.matmul_pop(accs[x][2 * t + 1])[:, :LANES]
            mean = total * (1.0 / M)
            spread = jnp.maximum(square * (1.0 / M) - mean * mean, 0.0)
            total_ref[p, pl.ds(t * PIECE, PIECE), :] = total
            scale_ref[p, pl.ds(t * PIECE, PIECE), :] = 1.0 / jnp.sqrt(spread + SPREAD_FLOOR)

    def starts(c):
        if isinstance(c, int):
            return 2 * c, rows + 8 if c == chunks - 1 else half + 2 * c
        return 2 * c, jnp.where(c == chunks - 1, rows + 8, half + 2 * c)

    def push(p, c, register):
        for x, first in enumerate(starts(c)):
            tiles = hankel_tiles([points_ref[p, pl.ds(first + m, 1), :] for m in range(4)])
            rhs = jnp.concatenate(
                [
                    jnp.concatenate([tiles[0], tiles[1]], axis=1),
                    jnp.concatenate([tiles[1], tiles[2]], axis=1),
                ],
                axis=0,
            )
            pltpu.matmul_push_rhs(rhs, register, x)

    def finish(blocks, p):
        spot = lax.broadcasted_iota(jnp.int32, (1, LANES), 1)
        limit = lengths_ref[p] - M
        for a in range(blocks + 1):
            if a < blocks:
                block = acc_ref[pl.ds(a * LANES, LANES), :]
                best = jnp.max(block.T, axis=0, keepdims=True)
            else:
                block = acc_ref[pl.ds(a * LANES, 8), :]
                best = jnp.broadcast_to(jnp.max(block, axis=1, keepdims=True)[:1], (1, LANES))
            best = best * q_scale_ref[pl.ds(p * q_pad + a, 1), :] * (1.0 / M)
            row = jnp.where(a * LANES + spot <= limit, 2.0 * (1.0 - best), 0.0)
            rows_ref[pl.ds(p * q_rows + a, 1), :] = row

    def row(p, j):
        return pl.ds(pl.multiple_of(p * tall, PIECE) + j * PIECE, PIECE)

    def multiply(p, j, slot, register):
        lhs = left_ref[row(p, j), :]
        for x in range(2):
            pltpu.matmul_acc_lhs(accs[x][slot], lhs, load_staged_rhs=register)

    def weights(p, c):
        at = [first + n for first in starts(c) for n in range(2)]
        return [[ref[p, pl.ds(r, 1), :] for r in at] for ref in (total_ref, scale_ref)]

    def fold(p, j, slot, totals, scales):
        mean = mean_ref[row(p, j), :]
        popped = [pltpu.matmul_pop(accs[x][slot]) for x in range(2)]
        at = pl.ds(j * PIECE, PIECE)
        best = acc_ref[at, :]
        for n in range(CHUNK):
            piece = popped[n // 2][:, (n % 2) * LANES : (n % 2 + 1) * LANES]
            best = jnp.maximum(best, (piece - mean * totals[n]) * scales[n])
        acc_ref[at, :] = best

    def pending(p, pieces, c, slots):
        known = []

        def one(s):
            if not known:
                known.append(weights(p, c))
            fold(p, s % pieces, s % slots, *known[0])

        return [functools.partial(one, s) for s in range(pieces)]

    def begin(pieces):
        rest = pl.ds(0, pieces * PIECE)
        acc_ref[rest, :] = jnp.full((pieces * PIECE, LANES), MASKED, jnp.float32)

    def visit_short(pieces, p, then, todo, close, ready):
        total = chunks * pieces
        slots = len(accs[0]) // pieces * pieces
        known = {}

        def one(s):
            c = s // pieces
            if c not in known:
                known[c] = weights(p, c)
            fold(p, s % pieces, s % slots, *known[c])

        ours = [functools.partial(one, s) for s in range(total)]
        lag = len(todo) or LAG
        for s in range(total):
            c, j = s // pieces, s % pieces
            if s >= ready:
                multiply(p, j, s % slots, None if j else c % 2)
            if s == 0:
                push(p, 1, 1)
            if j == 0 and c + 2 < chunks:
                push(p, c + 2, c % 2)
            if j == 0 and c + 2 == chunks and then is not None:
                push(then, 0, 0)
            if s < len(todo):
                todo[s]()
            if s + 1 == lag:
                close()
                begin(pieces)
            if s >= lag:
                ours[s - lag]()
        return ours[total - lag :]

    def visit_long(pieces, p, then, todo, close, ready):
        lag = min(LAG, pieces - 4)

        def pushes(c):
            if then is None:
                push(p, jnp.minimum(c, chunks - 1), 0)
            else:
                ends = c == chunks
                push(jnp.where(ends, then, p), jnp.where(ends, 0, c), 0)

        skip = len(todo) or lag
        ours = pending(p, pieces, 0, pieces)
        for s in range(pieces):
            if s >= ready:
                multiply(p, s, s, None if s else 0)
            if s == 0:
                push(p, 1, 0)
            if s < len(todo):
                todo[s]()
            if s + 1 == skip:
                close()
                begin(pieces)
            if s >= skip:
                ours[s - skip]()
        if skip > pieces:
            for step in todo[pieces:]:
                step()
            close()
            begin(pieces)
        for s in range(max(pieces - skip, 0), pieces - lag):
            ours[s]()

        @pl.loop(1, chunks)
        def _(c):
            before, ours = pending(p, pieces, c - 1, pieces), pending(p, pieces, c, pieces)
            both = before[pieces - lag :] + ours
            for s in range(pieces):
                multiply(p, s, s, None if s else 0)
                if s == 0:
                    pushes(c + 1)
                both[s]()

        return pending(p, pieces, chunks - 1, pieces)[pieces - lag :]

    def run(sizes, order):
        todo, close = [], lambda: None
        for n, (blocks, p) in enumerate(zip(sizes, order)):
            then = order[n + 1] if n + 1 < len(order) else None
            pieces = blocks * (LANES // PIECE) + 1
            visit = visit_short if pieces <= SHORT else visit_long
            todo = visit(pieces, p, then, todo, close, 0 if n else early)
            close = functools.partial(finish, blocks, p)
        for step in todo:
            step()
        close()
        if pieces > SHORT:
            for x in range(2):
                pltpu.matmul_acc_lhs(accs[x][0], left_ref[pl.ds(0, PIECE), :], load_staged_rhs=0)
                pltpu.matmul_pop(accs[x][0])

    rows_ref[...] = jnp.zeros(rows_ref.shape, jnp.float32)
    levels = [full // 3, full - 2, full - 1, full]
    blocks = [(lengths_ref[p] - M + LANES - 1) // LANES for p in range(per_device)]
    swap = blocks[1] > blocks[0]
    first, second = jnp.where(swap, 1, 0), jnp.where(swap, 0, 1)
    more, less = jnp.maximum(*blocks), jnp.minimum(*blocks)
    more, less = (
        sum((v > level).astype(jnp.int32) for level in levels[:-1]) for v in (more, less)
    )
    push(first, 0, 0)
    early = levels[0] * (LANES // PIECE) + 1
    for s in range(early):
        multiply(first, s, s, None if s else 0)
    pairs = [(levels[m], levels[n]) for m in range(len(levels)) for n in range(m + 1)]
    lax.switch(
        more * (more + 1) // 2 + less,
        [functools.partial(run, pair) for pair in pairs],
        (first, second),
    )
    for p in range(per_device):
        for a in range(q_rows):
            out_ref[pl.ds(p, 1), pl.ds(a * LANES, LANES)] = rows_ref[pl.ds(p * q_rows + a, 1), :]


def join(members, groups, lengths, queries, block):
    per_device, series_len = queries.shape
    rows = block.shape[0]
    q_rows = series_len // LANES
    tall = (series_len - M) // LANES * LANES + PIECE
    vmem = pl.BlockSpec(memory_space=pltpu.VMEM)
    smem = pl.BlockSpec(memory_space=pltpu.SMEM)
    gathered = pl.pallas_call(
        functools.partial(gather_kernel, members),
        out_shape=(
            pltpu.VMEM((members + 1, rows, LANES), jnp.bfloat16),
            pltpu.VMEM((per_device * tall, M), jnp.bfloat16),
            pltpu.VMEM((per_device * tall, LANES), jnp.float32),
            pltpu.VMEM((per_device * (q_rows + 8), LANES), jnp.float32),
            pltpu.VMEM((2, WIDE, WIDE), jnp.bfloat16),
            pltpu.SMEM((per_device,), jnp.int32),
            pltpu.SMEM((per_device,), jnp.int32),
        ),
        in_specs=[pl.BlockSpec(memory_space=pl.ANY)] * 4,
        out_specs=(vmem,) * 5 + (smem,) * 2,
        scratch_shapes=[
            pltpu.VMEM((per_device, series_len), jnp.bfloat16),
            pltpu.SemaphoreType.DMA((4,)),
            pltpu.SemaphoreType.DMA((1,)),
            pltpu.SemaphoreType.DMA((1,)),
        ],
        compiler_params=pltpu.CompilerParams(
            collective_id=0, has_side_effects=True
        ),
        name="gather",
    )(groups, lengths, queries, block)
    spaces = (pltpu.VMEM,) * 5 + (pltpu.SMEM,) * 2
    held = [pltpu.with_memory_space_constraint(x, space) for x, space in zip(gathered, spaces)]
    return pl.pallas_call(
        join_kernel,
        out_shape=jax.ShapeDtypeStruct((per_device, series_len), jnp.float32),
        in_specs=[vmem] * 5 + [smem] * 2,
        out_specs=vmem,
        scratch_shapes=[
            pltpu.VMEM((per_device, rows + 24, LANES), jnp.float32),
            pltpu.VMEM((per_device, rows + PIECE, LANES), jnp.float32),
            pltpu.VMEM((per_device, rows + PIECE, LANES), jnp.float32),
            pltpu.VMEM((tall, LANES), jnp.float32),
            pltpu.VMEM((per_device * q_rows + 8, LANES), jnp.float32),
        ],
        compiler_params=pltpu.CompilerParams(

        ),
        name="join",
    )(*held)


def body(long_series, queries, lengths, groups):
    members = lax.axis_size("ref")
    return join(members, groups, lengths, queries, long_series.reshape(-1, LANES))


def solution(mesh):
    in_specs = (
        P(("groups", "ref")),
        P(("groups", "ref"), None),
        P(("groups", "ref")),
        P(("groups", "ref")),
    )
    out_specs = P(("groups", "ref"), None)
    return jax.shard_map(body, mesh=mesh, in_specs=in_specs, out_specs=out_specs, check_vma=False)
```

```python
import functools

import jax
import jax.numpy as jnp
from jax import lax
from jax.experimental import pallas as pl
from jax.experimental.pallas import tpu as pltpu
from jax.sharding import PartitionSpec as P

M = 256
LANES = 128
WIDE = 2 * LANES
SPREAD_FLOOR = 0.25
CHUNK = 4
PIECE = 16
SHORT = 17
LAG = 28
MASKED = -1e30


def iotas(shape):
    return (
        lax.broadcasted_iota(jnp.int32, shape, 0),
        lax.broadcasted_iota(jnp.int32, shape, 1),
    )


def hankel_tiles(rows):
    shape = (LANES, LANES)
    sub, lane = iotas(shape)
    rolled = [
        pltpu.roll(
            jnp.broadcast_to(row, shape).astype(jnp.bfloat16), 1, 1, stride=1, stride_axis=0
        )
        for row in rows
    ]
    return [
        jnp.where(lane <= sub, here, there) for here, there in zip(rolled, rolled[1:])
    ]


def toeplitz(row, following):
    shape = (LANES, LANES)
    sub, lane = iotas(shape)
    here = pltpu.roll(jnp.broadcast_to(row, shape), 0, 1, stride=1, stride_axis=0)
    there = pltpu.roll(jnp.broadcast_to(following, shape), 0, 1, stride=1, stride_axis=0)
    return jnp.where(lane >= sub, here, there)


def next_row(x):
    return pltpu.roll(x, x.shape[0] - 1, 0)


def window_scale(x):
    lane = lax.broadcasted_iota(jnp.int32, x.shape, 1)
    total, square = x, jnp.zeros_like(x)
    count = 1
    while count < M:
        def ahead(v):
            if count == LANES:
                return next_row(v)
            rolled = pltpu.roll(v, LANES - count, 1)
            return jnp.where(lane < LANES - count, rolled, next_row(rolled))

        total_ahead, square_ahead = ahead(total), ahead(square)
        gap = total - total_ahead
        square = square + square_ahead + gap * gap * (0.5 / count)
        total = total + total_ahead
        count *= 2
    return 1.0 / jnp.sqrt(square * (1.0 / M) + SPREAD_FLOOR)


def gather_kernel(members, groups_hbm, lengths_hbm, q_hbm, block_hbm,
                  series_ref, left_ref, mean_ref, q_scale_ref, band_ref, groups_ref, lengths_ref,
                  q_ref, local_sem, send_sem, recv_sem):
    pieces = left_ref.shape[0] // lengths_ref.shape[0] // PIECE
    specs = [pltpu.ACC(x)((PIECE, WIDE), jnp.float32) for x in range(2) for _ in range(pieces)]

    def main(*accs):
        gather_body(members, groups_hbm, lengths_hbm, q_hbm, block_hbm,
                    series_ref, left_ref, mean_ref, q_scale_ref, band_ref, groups_ref, lengths_ref,
                    q_ref, local_sem, send_sem, recv_sem, (accs[:pieces], accs[pieces:]))

    pl.run_scoped(main, *specs)


def gather_body(members, groups_hbm, lengths_hbm, q_hbm, block_hbm,
                series_ref, left_ref, mean_ref, q_scale_ref, band_ref, groups_ref, lengths_ref,
                q_ref, local_sem, send_sem, recv_sem, accs):
    per_device, series_len = q_ref.shape
    q_rows = series_len // LANES
    rows = block_hbm.shape[0]
    full = (series_len - M) // LANES
    tall = left_ref.shape[0] // per_device
    pieces = tall // PIECE
    q_pad = q_rows + 8
    me = lax.axis_index("ref")

    def place(d):
        return lax.rem(me + d, members)

    def copy(src, d):
        return pltpu.make_async_remote_copy(
            src_ref=src, dst_ref=src, send_sem=send_sem.at[0], recv_sem=recv_sem.at[0],
            device_id={"ref": place(d)}, device_id_type=pl.DeviceIdType.MESH,
        )

    fetches = [
        pltpu.make_async_copy(block_hbm, series_ref.at[me], local_sem.at[0]),
        pltpu.make_async_copy(q_hbm, q_ref, local_sem.at[1]),
        pltpu.make_async_copy(groups_hbm, groups_ref, local_sem.at[2]),
        pltpu.make_async_copy(lengths_hbm, lengths_ref, local_sem.at[3]),
    ]
    barrier = pltpu.get_barrier_semaphore()
    for fetch in fetches:
        fetch.start()

    @pl.loop(1, members)
    def _(d):
        pl.semaphore_signal(
            barrier, inc=1, device_id={"ref": place(d)}, device_id_type=pl.DeviceIdType.MESH
        )

    series_ref[members] = jnp.zeros((rows, LANES), jnp.bfloat16)
    fetches[0].wait()
    pl.semaphore_wait(barrier, members - 1)

    @pl.loop(1, members)
    def _(d):
        copy(series_ref.at[me], d).start()

    fetches[1].wait()
    fetches[2].wait()
    fetches[3].wait()

    sub, lane = iotas((WIDE, WIDE))
    flip = jnp.where(sub + lane == LANES - 1, 1.0, 0.0).astype(jnp.bfloat16)
    ones = jnp.full((WIDE, WIDE), 1.0 / M, jnp.bfloat16)
    q_all = q_ref[...].astype(jnp.float32)
    parts = []
    for p in range(per_device):
        row_list = [q_all[p : p + 1, LANES * a : LANES * (a + 1)] for a in range(q_rows)]
        parts += row_list + [jnp.zeros((q_pad - q_rows, LANES), jnp.float32)]
    q_points = jnp.concatenate(parts, axis=0)
    q_scale_ref[...] = window_scale(q_points)
    q_lhs = jnp.concatenate([q_points, jnp.zeros_like(q_points)], axis=1).astype(jnp.bfloat16)
    pltpu.matmul_push_rhs(flip, 0, 0)
    for p in range(per_device):
        pltpu.matmul_acc_lhs(
            accs[0][p], q_lhs[p * q_pad : (p + 1) * q_pad], load_staged_rhs=None if p else 0
        )
    for x in range(2):
        pltpu.matmul_push_rhs(ones, 0, x)
    for p in range(per_device):
        q_back = pltpu.matmul_pop(accs[0][p])[:, :LANES]
        for a in range(full + 2):
            tile = toeplitz(q_back[a : a + 1], q_back[a + 1 : a + 2]).astype(jnp.bfloat16)
            for h in range(2):
                if 0 <= a - h < full:
                    left_ref[pl.ds(p * tall + (a - h) * LANES, LANES), pl.ds(h * LANES, LANES)] = tile
                elif a - h == full:
                    left_ref[pl.ds(p * tall + full * LANES, PIECE), pl.ds(h * LANES, LANES)] = tile[:PIECE]
    for p in range(per_device):
        for i in range(pieces):
            x = i % 2
            pltpu.matmul_acc_lhs(
                accs[x][i], left_ref[pl.ds(p * tall + i * PIECE, PIECE), :],
                load_staged_rhs=0 if p == 0 and i < 2 else None,
            )
        for i in range(pieces):
            mean_ref[pl.ds(p * tall + i * PIECE, PIECE), :] = pltpu.matmul_pop(accs[i % 2][i])[:, :LANES]

    band_ref[0] = jnp.where(
        (lane >= LANES) | (sub >= LANES) | (sub >= lane), 1.0, 0.0
    ).astype(jnp.bfloat16)
    band_ref[1] = jnp.where((sub < LANES) & (sub < lane), 1.0, 0.0).astype(jnp.bfloat16)

    whole = series_ref.at[pl.ds(0, members - 1)]
    copy(whole, 1).wait_recv()
    copy(whole, 1).wait_send()


def join_kernel(series_ref, left_ref, mean_ref, q_scale_ref, band_ref, groups_ref, lengths_ref,
                out_ref, points_ref, total_ref, scale_ref, first_ref, second_ref, rows_ref):
    slots = 60
    specs = [pltpu.ACC(x)((PIECE, WIDE), jnp.float32) for x in range(2) for _ in range(slots)]

    def main(*accs):
        join_body(series_ref, left_ref, mean_ref, q_scale_ref, band_ref, groups_ref, lengths_ref,
                  out_ref, points_ref, total_ref, scale_ref, (first_ref, second_ref), rows_ref,
                  (accs[:slots], accs[slots:]))

    pl.run_scoped(main, *specs)


def join_body(series_ref, left_ref, mean_ref, q_scale_ref, band_ref, groups_ref, lengths_ref,
              out_ref, points_ref, total_ref, scale_ref, acc_refs, rows_ref, accs):
    per_device, series_len = out_ref.shape
    members, rows = series_ref.shape[0] - 1, series_ref.shape[1]
    q_rows = series_len // LANES
    q_pad = q_rows + 8
    full = (series_len - M) // LANES
    tall = left_ref.shape[0] // per_device
    chunks = rows // CHUNK
    half = rows // 2

    for x in range(2):
        for r in range(2):
            pltpu.matmul_push_rhs(band_ref[r], r, x)

    for p in range(per_device):
        g = groups_ref[p]
        block = series_ref[g].astype(jnp.float32)
        ahead = series_ref[g + 1].astype(jnp.float32)
        points_ref[p, pl.ds(0, rows), :] = block
        points_ref[p, pl.ds(rows, 8), :] = ahead[:8]
        shape = (8, LANES)
        spot = lax.broadcasted_iota(jnp.int32, shape, 1)
        tail = jnp.concatenate([block[rows - 2 :], ahead[:6]], axis=0)
        moved = pltpu.roll(block[rows - 8 :], LANES - 1, 1)
        moved = jnp.where(spot < LANES - 1, moved, next_row(moved))
        moved = jnp.concatenate([moved[4:], moved[:4]], axis=0)
        final = jnp.full(shape, g, jnp.int32) == members - 1
        points_ref[p, pl.ds(rows + 8, 8), :] = jnp.where(final, moved, tail)
        points_ref[p, pl.ds(rows + 16, 8), :] = jnp.zeros(shape, jnp.float32)
    for p in range(per_device):
        x = p % 2
        here, ahead, beyond = (points_ref[p, pl.ds(s, rows + PIECE), :] for s in range(3))

        def operand(f):
            close = jnp.concatenate([f(here), f(ahead)], axis=1)
            away = jnp.concatenate([f(beyond), jnp.zeros_like(f(beyond))], axis=1)
            return close, away

        def high(v):
            return (v * v).astype(jnp.bfloat16)

        def low(v):
            return (v * v - high(v).astype(jnp.float32)).astype(jnp.bfloat16)

        plain = operand(lambda v: v.astype(jnp.bfloat16))
        squares = [operand(high), operand(low)]
        stat_pieces = rows // PIECE + 1
        for s in range(2):
            for t in range(stat_pieces):
                cut = slice(t * PIECE, (t + 1) * PIECE)
                pltpu.matmul_acc_lhs(
                    accs[x][2 * t], plain[s][cut], load_staged_rhs=s if t == 0 else None
                )
                for square in squares:
                    pltpu.matmul_acc_lhs(accs[x][2 * t + 1], square[s][cut])
        for t in range(stat_pieces):
            total = pltpu.matmul_pop(accs[x][2 * t])[:, :LANES]
            square = pltpu.matmul_pop(accs[x][2 * t + 1])[:, :LANES]
            mean = total * (1.0 / M)
            spread = jnp.maximum(square * (1.0 / M) - mean * mean, 0.0)
            total_ref[p, pl.ds(t * PIECE, PIECE), :] = total
            scale_ref[p, pl.ds(t * PIECE, PIECE), :] = 1.0 / jnp.sqrt(spread + SPREAD_FLOOR)

    def starts(c):
        if isinstance(c, int):
            return 2 * c, rows + 8 if c == chunks - 1 else half + 2 * c
        return 2 * c, jnp.where(c == chunks - 1, rows + 8, half + 2 * c)

    def push(p, c, register):
        for x, first in enumerate(starts(c)):
            tiles = hankel_tiles([points_ref[p, pl.ds(first + m, 1), :] for m in range(4)])
            rhs = jnp.concatenate(
                [
                    jnp.concatenate([tiles[0], tiles[1]], axis=1),
                    jnp.concatenate([tiles[1], tiles[2]], axis=1),
                ],
                axis=0,
            )
            pltpu.matmul_push_rhs(rhs, register, x)

    def finish(acc, blocks, p):
        spot = lax.broadcasted_iota(jnp.int32, (1, LANES), 1)
        limit = lengths_ref[p] - M
        for a in range(blocks + 1):
            if a < blocks:
                block = acc[pl.ds(a * LANES, LANES), :]
                best = jnp.max(block.T, axis=0, keepdims=True)
            else:
                block = acc[pl.ds(a * LANES, 8), :]
                best = jnp.broadcast_to(jnp.max(block, axis=1, keepdims=True)[:1], (1, LANES))
            best = best * q_scale_ref[pl.ds(p * q_pad + a, 1), :] * (1.0 / M)
            row = jnp.where(a * LANES + spot <= limit, 2.0 * (1.0 - best), 0.0)
            rows_ref[pl.ds(p * q_rows + a, 1), :] = row

    def row(p, j):
        return pl.ds(pl.multiple_of(p * tall, PIECE) + j * PIECE, PIECE)

    def multiply(p, j, slot, register):
        lhs = left_ref[row(p, j), :]
        for x in range(2):
            pltpu.matmul_acc_lhs(accs[x][slot], lhs, load_staged_rhs=register)

    def weights(p, c):
        at = [first + n for first in starts(c) for n in range(2)]
        return [[ref[p, pl.ds(r, 1), :] for r in at] for ref in (total_ref, scale_ref)]

    def fold(acc, p, j, slot, totals, scales):
        mean = mean_ref[row(p, j), :]
        popped = [pltpu.matmul_pop(accs[x][slot]) for x in range(2)]
        at = pl.ds(j * PIECE, PIECE)
        best = acc[at, :]
        for n in range(CHUNK):
            piece = popped[n // 2][:, (n % 2) * LANES : (n % 2 + 1) * LANES]
            best = jnp.maximum(best, (piece - mean * totals[n]) * scales[n])
        acc[at, :] = best

    def pending(acc, p, pieces, c, slots):
        known = []

        def one(s):
            if not known:
                known.append(weights(p, c))
            fold(acc, p, s % pieces, s % slots, *known[0])

        return [functools.partial(one, s) for s in range(pieces)]

    def begin(acc, pieces):
        rest = pl.ds(0, pieces * PIECE)
        acc[rest, :] = jnp.full((pieces * PIECE, LANES), MASKED, jnp.float32)

    def visit_short(acc, pieces, p, then, todo, ready):
        total = chunks * pieces
        slots = len(accs[0]) // pieces * pieces
        known = {}

        def one(s):
            c = s // pieces
            if c not in known:
                known[c] = weights(p, c)
            fold(acc, p, s % pieces, s % slots, *known[c])

        ours = [functools.partial(one, s) for s in range(total)]
        lag = len(todo) or LAG
        begin(acc, pieces)
        for s in range(total):
            c, j = s // pieces, s % pieces
            if s >= ready:
                multiply(p, j, s % slots, None if j else c % 2)
            if s == 0:
                push(p, 1, 1)
            if j == 0 and c + 2 < chunks:
                push(p, c + 2, c % 2)
            if j == 0 and c + 2 == chunks and then is not None:
                push(then, 0, 0)
            if s < len(todo):
                todo[s]()
            if s >= lag:
                ours[s - lag]()
        return ours[total - lag :]

    def visit_long(acc, pieces, p, then, todo, ready):
        lag = min(LAG, pieces - 4)

        def pushes(c):
            if then is None:
                push(p, jnp.minimum(c, chunks - 1), 0)
            else:
                ends = c == chunks
                push(jnp.where(ends, then, p), jnp.where(ends, 0, c), 0)

        skip = len(todo) or lag
        begin(acc, pieces)
        ours = pending(acc, p, pieces, 0, pieces)
        for s in range(pieces):
            if s >= ready:
                multiply(p, s, s, None if s else 0)
            if s == 0:
                push(p, 1, 0)
            if s < len(todo):
                todo[s]()
            if s >= skip:
                ours[s - skip]()
        if skip > pieces:
            for step in todo[pieces:]:
                step()
        for s in range(max(pieces - skip, 0), pieces - lag):
            ours[s]()

        @pl.loop(1, chunks)
        def _(c):
            before, ours = pending(acc, p, pieces, c - 1, pieces), pending(acc, p, pieces, c, pieces)
            both = before[pieces - lag :] + ours
            for s in range(pieces):
                multiply(p, s, s, None if s else 0)
                if s == 0:
                    pushes(c + 1)
                both[s]()

        return pending(acc, p, pieces, chunks - 1, pieces)[pieces - lag :]

    def run(sizes, order):
        todo = []
        for n, (blocks, p) in enumerate(zip(sizes, order)):
            then = order[n + 1] if n + 1 < len(order) else None
            pieces = blocks * (LANES // PIECE) + 1
            visit = visit_short if pieces <= SHORT else visit_long
            todo = visit(acc_refs[n], pieces, p, then, todo, 0 if n else early)
        for n, step in enumerate([*todo, None]):
            if n == 0:
                for acc, blocks, p in list(zip(acc_refs, sizes, order))[:-1]:
                    finish(acc, blocks, p)
            if step:
                step()
        finish(acc_refs[len(sizes) - 1], sizes[-1], order[-1])
        if pieces > SHORT:
            for x in range(2):
                pltpu.matmul_acc_lhs(accs[x][0], left_ref[pl.ds(0, PIECE), :], load_staged_rhs=0)
                pltpu.matmul_pop(accs[x][0])

    rows_ref[...] = jnp.zeros(rows_ref.shape, jnp.float32)
    levels = [full // 3, full - 2, full - 1, full]
    blocks = [(lengths_ref[p] - M + LANES - 1) // LANES for p in range(per_device)]
    swap = blocks[1] > blocks[0]
    first, second = jnp.where(swap, 1, 0), jnp.where(swap, 0, 1)
    more, less = jnp.maximum(*blocks), jnp.minimum(*blocks)
    more, less = (
        sum((v > level).astype(jnp.int32) for level in levels[:-1]) for v in (more, less)
    )
    push(first, 0, 0)
    early = levels[0] * (LANES // PIECE) + 1
    for s in range(early):
        multiply(first, s, s, None if s else 0)
    pairs = [(levels[m], levels[n]) for m in range(len(levels)) for n in range(m + 1)]
    lax.switch(
        more * (more + 1) // 2 + less,
        [functools.partial(run, pair) for pair in pairs],
        (first, second),
    )
    for p in range(per_device):
        for a in range(q_rows):
            out_ref[pl.ds(p, 1), pl.ds(a * LANES, LANES)] = rows_ref[pl.ds(p * q_rows + a, 1), :]


def join(members, groups, lengths, queries, block):
    per_device, series_len = queries.shape
    rows = block.shape[0]
    q_rows = series_len // LANES
    tall = (series_len - M) // LANES * LANES + PIECE
    vmem = pl.BlockSpec(memory_space=pltpu.VMEM)
    smem = pl.BlockSpec(memory_space=pltpu.SMEM)
    gathered = pl.pallas_call(
        functools.partial(gather_kernel, members),
        out_shape=(
            pltpu.VMEM((members + 1, rows, LANES), jnp.bfloat16),
            pltpu.VMEM((per_device * tall, M), jnp.bfloat16),
            pltpu.VMEM((per_device * tall, LANES), jnp.float32),
            pltpu.VMEM((per_device * (q_rows + 8), LANES), jnp.float32),
            pltpu.VMEM((2, WIDE, WIDE), jnp.bfloat16),
            pltpu.SMEM((per_device,), jnp.int32),
            pltpu.SMEM((per_device,), jnp.int32),
        ),
        in_specs=[pl.BlockSpec(memory_space=pl.ANY)] * 4,
        out_specs=(vmem,) * 5 + (smem,) * 2,
        scratch_shapes=[
            pltpu.VMEM((per_device, series_len), jnp.bfloat16),
            pltpu.SemaphoreType.DMA((4,)),
            pltpu.SemaphoreType.DMA((1,)),
            pltpu.SemaphoreType.DMA((1,)),
        ],
        compiler_params=pltpu.CompilerParams(
            collective_id=0, has_side_effects=True
        ),
        name="gather",
    )(groups, lengths, queries, block)
    spaces = (pltpu.VMEM,) * 5 + (pltpu.SMEM,) * 2
    held = [pltpu.with_memory_space_constraint(x, space) for x, space in zip(gathered, spaces)]
    return pl.pallas_call(
        join_kernel,
        out_shape=jax.ShapeDtypeStruct((per_device, series_len), jnp.float32),
        in_specs=[vmem] * 5 + [smem] * 2,
        out_specs=vmem,
        scratch_shapes=[
            pltpu.VMEM((per_device, rows + 24, LANES), jnp.float32),
            pltpu.VMEM((per_device, rows + PIECE, LANES), jnp.float32),
            pltpu.VMEM((per_device, rows + PIECE, LANES), jnp.float32),
            pltpu.VMEM((tall, LANES), jnp.float32),
            pltpu.VMEM((tall, LANES), jnp.float32),
            pltpu.VMEM((per_device * q_rows + 8, LANES), jnp.float32),
        ],
        compiler_params=pltpu.CompilerParams(

        ),
        name="join",
    )(*held)


def body(long_series, queries, lengths, groups):
    members = lax.axis_size("ref")
    return join(members, groups, lengths, queries, long_series.reshape(-1, LANES))


def solution(mesh):
    in_specs = (
        P(("groups", "ref")),
        P(("groups", "ref"), None),
        P(("groups", "ref")),
        P(("groups", "ref")),
    )
    out_specs = P(("groups", "ref"), None)
    return jax.shard_map(body, mesh=mesh, in_specs=in_specs, out_specs=out_specs, check_vma=False)
```
